256 devices in a mesh: row: 8 (over y, x_lo), col: 32 (over z, x_hi, core).
Axes of the slice: x: 4 (x_hi: 2, x_lo: 2; x = x_hi * 2 + x_lo), y: 4, z: 8, core: 2. Of those that a mesh axis runs over, the one named last changes fastest.
Arguments:
- pair_rep: bfloat16 [1024, 1024, 128], P('row', 'col'), may hold values from -6 to 6
- proj_weight: bfloat16 [2, 4, 128, 128], replicated, may hold values from -0.5 to 0.5
- gate_weight: bfloat16 [2, 128, 128], replicated, may hold values from -0.5 to 0.5
- out_weight: bfloat16 [2, 128, 128], replicated, may hold values from -0.5 to 0.5
- in_gain: float32 [2, 128], replicated, may hold values from 0.1 to 1.9
- out_gain: float32 [2, 128], replicated, may hold values from 0.1 to 1.9
Outputs:
- updated_pair: bfloat16 [1024, 1024, 128], P('row', 'col')
The draws below stay inside these ranges and needn't reach their ends.
All inputs are finite; a program needn't handle non-finite values.
Results may differ from the reference program's by a relative error of at most 0.011.
Values may be sent and summed in bfloat16 or wider, within the bound.
A program may use at most 64 MiB of HBM per device.

```python
import math
import jax
import jax.numpy as jnp
from jax import lax

C = 128
H = 128
N = 1024


def steps_of(own_key, extent, cuts, smallest, largest):
    def one(position, parts):
        draws = jax.random.uniform(jax.random.fold_in(jax.random.fold_in(own_key, 6), position), (parts,), jnp.float32, smallest / len(cuts), largest / len(cuts))
        return jnp.repeat(jnp.exp(draws), extent[position] // parts).reshape((-1,) + (1,) * (len(extent) - position - 1))

    level = one(*cuts[0])
    for cut in cuts[1:]:
        level = level * one(*cut)
    return level


def noise(key, extent, deviation, most, cuts=(), kind=jnp.bfloat16):
    entries = jax.random.normal(key, extent, jnp.float32) * deviation
    if len(cuts) > 0:
        entries = steps_of(key, extent, cuts, -0.22, 0.18) * entries
    return jnp.clip(entries, min=-most, max=most).astype(kind)


def setup_inputs(seed: int = 0) -> dict:
    arg_keys = jax.random.split(jax.random.key(seed), 7)
    pair_rep = noise(arg_keys[0], (N, N, C), 1.0, 6.0, ((0, 8), (1, 32)))
    proj_weight = noise(arg_keys[1], (2, 4, C, H), C ** -0.5, 0.5)
    gate_weight = noise(arg_keys[2], (2, C, C), C ** -0.5, 0.5)
    out_weight = noise(arg_keys[3], (2, H, C), H ** -0.5, 0.5)
    in_gain = jnp.clip(1.0 + 0.18 * jax.random.normal(arg_keys[4], (2, C), jnp.float32), 0.1, 1.9)
    out_gain = jnp.clip(1.0 + 0.18 * jax.random.normal(arg_keys[5], (2, H), jnp.float32), 0.1, 1.9)
    return dict(pair_rep=pair_rep, proj_weight=proj_weight, gate_weight=gate_weight, out_weight=out_weight, in_gain=in_gain, out_gain=out_gain)


epsilon = 1e-05

def layer_norm(values, gain_row):
    center = values - lax.optimization_barrier(jnp.mean(values, axis=-1, keepdims=True))
    spread = lax.optimization_barrier(jnp.mean(center * center, axis=-1, keepdims=True))
    return center * lax.rsqrt(spread + epsilon) * gain_row

def reference(pair_rep, proj_weight, gate_weight, out_weight, in_gain, out_gain):
    row_block = math.gcd(N, 64)
    channel_block = math.gcd(H, 16)
    current = pair_rep
    for update_index in range(2):
        weight_joined = jnp.transpose(proj_weight[update_index], (1, 0, 2)).reshape(C, 4 * H)

        def project(row_slab):
            widened = row_slab.astype(jnp.float32)
            normed = layer_norm(widened, in_gain[update_index]).astype(jnp.bfloat16)
            projected = jnp.dot(normed, weight_joined, preferred_element_type=jnp.float32)
            left_hand = (jax.nn.sigmoid(projected[..., 0:H]) * projected[..., H:2 * H]).astype(jnp.bfloat16)
            right_hand = (jax.nn.sigmoid(projected[..., 2 * H:3 * H]) * projected[..., 3 * H:4 * H]).astype(jnp.bfloat16)
            gating = jax.nn.sigmoid(jnp.dot(normed, gate_weight[update_index], preferred_element_type=jnp.float32))
            return (left_hand, right_hand, gating)
        blocks = current.reshape(N // row_block, row_block, N, C)
        left_hand, right_hand, gating = lax.map(project, blocks)
        left_channels = jnp.moveaxis(left_hand.reshape(N, N, H), 2, 0).reshape(H // channel_block, channel_block, N, N)
        right_channels = jnp.moveaxis(right_hand.reshape(N, N, H), 2, 0).reshape(H // channel_block, channel_block, N, N)
        pattern = 'hik,hjk->hij' if update_index == 0 else 'hki,hkj->hij'

        def contract(operands):
            return jnp.einsum(pattern, operands[0].astype(jnp.float32), operands[1].astype(jnp.float32)).astype(jnp.bfloat16)
        triangle = lax.map(contract, (left_channels, right_channels))
        triangle = jnp.moveaxis(triangle.reshape(H, N, N), 0, 2)

        def finish(pieces):
            triangle_rows, gate_rows, old_rows = pieces
            mixed = layer_norm(triangle_rows.astype(jnp.float32), out_gain[update_index]).astype(jnp.bfloat16)
            update = jnp.dot(mixed, out_weight[update_index], preferred_element_type=jnp.float32)
            return (old_rows.astype(jnp.float32) + gate_rows * update).astype(jnp.bfloat16)
        current = lax.map(finish, (triangle.reshape(N // row_block, row_block, N, H), gating, blocks)).reshape(N, N, C)
    return current
```

```python
import functools

import jax
import jax.numpy as jnp
from jax import lax
from jax.experimental import pallas as pl
from jax.experimental.pallas import tpu as pltpu
from jax.sharding import PartitionSpec as P

EPS = 1e-05
MESH = pl.DeviceIdType.MESH
BF = jnp.bfloat16
F32 = jnp.float32
PITCH = 40
LANES = 512

STAGES = (
    "lz", "ly", "lx", "rx", "ry", "rz", "swap", "az", "ax", "ay", "bx", "by", "bz",
)


def scratch_of(update):
    whole, half = (32, 128), (16, 128)
    target = (2, 2, 8, 2, 2) if update == 0 else (4, 2, 4, 2, 2)
    return {
        "al": (8, 4, 4) + whole,
        "l1": (8, 4, 4) + whole,
        "l2": (4, 8, 4) + whole,
        "dl": target + whole,
        "ar": (8, 4, 4) + whole,
        "r1": (2, 2, 8, 4) + whole,
        "r2": (4, 2, 2, 8) + whole,
        "dr": (2, 2, 8, 2, 2) + whole,
        "ds": (2, 2, 8, 2, 2) + whole,
        "ta": (2, 2, 8, 2, 2) + half,
        "tb": (2, 2, 8, 2, 2) + half,
        "a1": (8, 2, 2, 2, 2) + half,
        "a2": (8, 4, 4) + half,
        "fa": (8, 4, 4) + half,
        "b1": (4, 4, 8) + half,
        "b2": (4, 4, 8) + half,
        "fb": (8, 4, 4) + half,
    }


NAMES = tuple(scratch_of(0))


def kernel(x_ref, pw_ref, gw_ref, ow_ref, ig_ref, og_ref, out_ref, *scratch):
    count = len(NAMES)
    buffers = [dict(zip(NAMES, scratch[u * count : (u + 1) * count])) for u in range(2)]
    wt, norm, gate, state, stage, right_t, acc, dummy, send_sem, recv_sem = scratch[2 * count :]

    row, col = lax.axis_index("row"), lax.axis_index("col")
    y, xl = lax.div(row, 2), lax.rem(row, 2)
    z, xh, core = lax.div(col, 4), lax.rem(lax.div(col, 2), 2), lax.rem(col, 2)
    x = xh * 2 + xl
    other = 1 - core

    def device(tx, ty, tz, tc):
        return (ty * 2 + lax.rem(tx, 2), tz * 4 + lax.div(tx, 2) * 2 + tc)

    def turned(own, by, size):
        return lax.rem(own + by, size)

    steps_z, steps_4 = (1, 7, 2, 6, 3, 5, 4), (1, 3, 2)

    barrier = pltpu.get_barrier_semaphore()
    peers = [device(x, y, z, other)]
    for t in (core, other):
        peers += [device(x, y, turned(z, d, 8), t) for d in steps_z]
        peers += [device(x, turned(y, d, 4), z, t) for d in steps_4]
        peers += [device(turned(x, d, 4), y, z, t) for d in steps_4]
    for peer in peers:
        pl.semaphore_signal(barrier, inc=1, device_id=peer, device_id_type=MESH)

    def send(update, name, src, dst, target):
        index = update * len(STAGES) + STAGES.index(name)
        pltpu.make_async_remote_copy(
            src_ref=src,
            dst_ref=dst,
            send_sem=send_sem.at[index],
            recv_sem=recv_sem.at[index],
            device_id=target,
            device_id_type=MESH,
        ).start()

    moved = dict(
        lz=112, ly=96, lx=112, rx=96, ry=96, rz=120, swap=128,
        az=56, ax=56, ay=48, bx=56, by=48, bz=56,
    )

    def descriptor(update, name):
        index = update * len(STAGES) + STAGES.index(name)
        whole = dummy.at[pl.ds(0, moved[name])]
        return pltpu.make_async_remote_copy(
            src_ref=whole,
            dst_ref=whole,
            send_sem=send_sem.at[index],
            recv_sem=recv_sem.at[index],
            device_id=device(x, y, z, other),
            device_id_type=MESH,
        )

    def arrived(update, name):
        descriptor(update, name).wait_recv()

    for u in range(2):
        for p in range(4):
            wt[u, p] = pw_ref[u, p].astype(F32).T.astype(BF)
        wt[u, 4] = gw_ref[u].astype(F32).T.astype(BF)
        wt[u, 5] = ow_ref[u].astype(F32).T.astype(BF)

    chunks = 4096 // LANES
    tiles = LANES // 128

    def lanes(step):
        return pl.ds(pl.multiple_of(step * LANES, LANES), LANES)

    def normalise(update, source):
        gain = jnp.broadcast_to(ig_ref[update : update + 1, :], (128, 128)).T
        gain = jnp.concatenate([gain] * tiles, axis=1)

        @pl.loop(0, chunks)
        def _(step):
            wide = source[:, lanes(step)].astype(F32)
            center = wide - jnp.mean(wide, axis=0, keepdims=True)
            spread = jnp.mean(center * center, axis=0, keepdims=True)
            norm[:, lanes(step)] = (center * lax.rsqrt(spread + EPS) * gain).astype(BF)

    def project(update, first, target):
        weight_gate, weight_value = wt[update, first], wt[update, first + 1]

        @pl.loop(0, chunks)
        def _(step):
            normed = norm[:, lanes(step)]
            opening = jnp.dot(weight_gate, normed, preferred_element_type=F32)
            value = jnp.dot(weight_value, normed, preferred_element_type=F32)
            hand = jax.nn.sigmoid(opening) * value
            for t in range(tiles):
                stage[pl.ds(step * tiles + t, 128, stride=PITCH), :] = hand[:, t * 128 : (t + 1) * 128]

        @pl.loop(0, 8)
        def _(hz):
            for hy in range(4):
                for hx in range(4):
                    start = pl.multiple_of(hz * 16 * PITCH + (hy * 4 + hx) * PITCH, 8)
                    target[hz, hy, hx] = stage[pl.ds(start, 32), :].astype(BF)

    def gates(update):
        weight = wt[update, 4]

        @pl.loop(0, chunks)
        def _(step):
            opening = jnp.dot(weight, norm[:, lanes(step)], preferred_element_type=F32)
            gate[:, lanes(step)] = jax.nn.sigmoid(opening)

    def contract_outgoing(b, half, right):
        left = b["dl"]
        for jb in range(4):
            block = right[jb // 2, jb % 2].reshape(1024, 128)
            right_t[pl.ds(jb * 128, 128), :] = block.T
        for yq in range(2):
            operand = jnp.concatenate(
                [left[yq, lo].reshape(1024, 128) for lo in range(2)], axis=1
            )
            product = jnp.dot(right_t[...], operand, preferred_element_type=F32).astype(BF)
            product = product.reshape(4, 2, 2, 2, 16, 256)
            for lo in range(2):
                piece = product[..., lo * 128 : (lo + 1) * 128]
                b["ta"][yq, lo, pl.ds(half * 4, 4)] = piece[:, :, :, 0]
                b["tb"][yq, lo, pl.ds(half * 4, 4)] = piece[:, :, :, 1]

    def contract_incoming(b, half, right, last):
        left = b["dl"]
        operand = jnp.concatenate(
            [left[half * 2 + kb // 2, kb % 2].reshape(512, 128) for kb in range(4)], axis=1
        )
        for part in range(4):
            zs = slice(part * 2, part * 2 + 2)
            rows = jnp.concatenate(
                [right[kb // 2, kb % 2, zs].reshape(256, 128) for kb in range(4)], axis=1
            )
            product = lax.dot_general(
                rows, operand, (((1,), (1,)), ((), ())), preferred_element_type=F32
            )
            here = slice(part * 256, part * 256 + 256)
            if not last:
                acc[here, :] = product
                continue
            total = (acc[here, :] + product).astype(BF).reshape(2, 2, 2, 2, 16, 512)
            for yq in range(2):
                for lo in range(2):
                    first = (yq * 2 + lo) * 128
                    piece = total[..., first : first + 128]
                    b["ta"][yq, lo, zs] = piece[:, :, :, 0]
                    b["tb"][yq, lo, zs] = piece[:, :, :, 1]

    def finish(update, source, j_half, old, new):
        def total(read):
            def add(hz, running):
                for hy in range(4):
                    for hx in range(4):
                        running = running + read(hz, hy, hx)
                return running

            return lax.fori_loop(0, 8, add, jnp.zeros((16, 128), F32))

        mean = total(lambda *h: source[h].astype(F32)) * (1.0 / 128)

        def square(*h):
            center = source[h].astype(F32) - mean
            return center * center

        inverse = lax.rsqrt(total(square) * (1.0 / 128) + EPS)

        @pl.loop(0, 8)
        def _(hz):
            for hy in range(4):
                for hx in range(4):
                    channel = hz * 16 + hy * 4 + hx
                    mixed = (source[hz, hy, hx].astype(F32) - mean) * inverse * og_ref[update, channel]
                    stage[pl.ds(pl.multiple_of(channel * PITCH, 8), 16), :] = mixed

        weight = wt[update, 5]

        for step in range(16 // tiles):
            mixed = jnp.concatenate(
                [stage[pl.ds(step * tiles + t, 128, stride=PITCH), :] for t in range(tiles)], axis=1
            ).astype(BF)
            change = jnp.dot(weight, mixed, preferred_element_type=F32)
            here = pl.ds(j_half * 2048 + step * LANES, LANES)
            new[:, here] = (old[:, here].astype(F32) + gate[:, here] * change).astype(BF)

    for u in range(2):
        b = buffers[u]
        old, new = (x_ref, state) if u == 0 else (state, out_ref)
        normalise(u, old)
        project(u, 0, b["al"])
        if u == 0:
            pl.semaphore_wait(barrier, len(peers))
        for d in steps_z:
            tz = turned(z, d, 8)
            send(u, "lz", b["al"].at[tz], b["l1"].at[z], device(x, y, tz, core))
        b["l1"][z] = b["al"][z]
        project(u, 2, b["ar"])
        for d in steps_4:
            tx = turned(x, d, 4)
            send(u, "rx", b["ar"].at[:, :, tx], b["r1"].at[xl, xh], device(tx, y, z, core))
        b["r1"][xl, xh] = b["ar"][:, :, x]
        gates(u)

        arrived(u, "rx")
        for d in steps_4:
            ty = turned(y, d, 4)
            send(u, "ry", b["r1"].at[:, :, :, ty], b["r2"].at[y], device(x, ty, z, core))
        b["r2"][y] = b["r1"][:, :, :, y]

        arrived(u, "lz")
        for d in steps_4:
            ty = turned(y, d, 4)
            send(u, "ly", b["l1"].at[:, ty], b["l2"].at[y], device(x, ty, z, core))
        b["l2"][y] = b["l1"][:, y]

        arrived(u, "ry")
        for d in steps_z:
            for t in (core, other):
                tz = turned(z, d, 8)
                send(
                    u, "rz", b["r2"].at[pl.ds(t * 2, 2), :, :, tz],
                    b["dr"].at[:, :, z, :, core], device(x, y, tz, t),
                )
        send(
            u, "rz", b["r2"].at[pl.ds(other * 2, 2), :, :, z],
            b["dr"].at[:, :, z, :, core], device(x, y, z, other),
        )
        b["dr"][:, :, z, :, core] = b["r2"][pl.ds(core * 2, 2), :, :, z]

        arrived(u, "ly")

        def left_of(t, tx):
            if u == 0:
                return b["l2"].at[pl.ds(t * 2, 2), :, tx]
            return b["l2"].at[:, pl.ds(t * 4, 4), tx]

        for d in steps_4:
            for t in (core, other):
                tx = turned(x, d, 4)
                send(u, "lx", left_of(t, tx), b["dl"].at[:, xl, :, xh, core], device(tx, y, z, t))
        send(u, "lx", left_of(other, x), b["dl"].at[:, xl, :, xh, core], device(x, y, z, other))
        b["dl"][:, xl, :, xh, core] = left_of(core, x)[...]

        arrived(u, "rz")
        send(u, "swap", b["dr"], b["ds"], device(x, y, z, other))
        arrived(u, "lx")
        if u == 0:
            contract_outgoing(b, core, b["dr"])
            arrived(u, "swap")
            contract_outgoing(b, other, b["ds"])
        else:
            contract_incoming(b, core, b["dr"], False)
            arrived(u, "swap")
            contract_incoming(b, other, b["ds"], True)

        for d in steps_z:
            tz = turned(z, d, 8)
            send(u, "az", b["ta"].at[:, :, tz], b["a1"].at[z], device(x, y, tz, core))
        for d in (1, 3, 2, 0):
            for t in (core, other):
                tx = turned(x, d, 4)
                tl, th = lax.rem(tx, 2), lax.div(tx, 2)
                if d == 0 and t is core:
                    continue
                send(
                    u, "bx", b["tb"].at[:, tl, :, th, t],
                    b["b1"].at[pl.ds(core * 2, 2), x], device(tx, y, z, t),
                )
        b["a1"][z] = b["ta"][:, :, z]
        b["b1"][pl.ds(core * 2, 2), x] = b["tb"][:, xl, :, xh, core]

        arrived(u, "bx")
        for d in steps_4:
            ty = turned(y, d, 4)
            send(u, "by", b["b1"].at[ty], b["b2"].at[y], device(x, ty, z, core))
        b["b2"][y] = b["b1"][y]

        arrived(u, "az")
        for d in (1, 3, 2, 0):
            for t in (core, other):
                tx = turned(x, d, 4)
                tl, th = lax.rem(tx, 2), lax.div(tx, 2)
                if d == 0 and t is core:
                    continue
                send(
                    u, "ax", b["a1"].at[:, :, tl, th, t],
                    b["a2"].at[:, pl.ds(core * 2, 2), x], device(tx, y, z, t),
                )
        b["a2"][:, pl.ds(core * 2, 2), x] = b["a1"][:, :, xl, xh, core]

        arrived(u, "by")
        for d in steps_z:
            tz = turned(z, d, 8)
            send(u, "bz", b["b2"].at[:, :, tz], b["fb"].at[z], device(x, y, tz, core))
        b["fb"][z] = b["b2"][:, :, z]

        arrived(u, "ax")
        for d in steps_4:
            ty = turned(y, d, 4)
            send(u, "ay", b["a2"].at[:, ty], b["fa"].at[:, y], device(x, ty, z, core))
        b["fa"][:, y] = b["a2"][:, y]

        arrived(u, "ay")
        finish(u, b["fa"], 0, old, new)
        arrived(u, "bz")
        finish(u, b["fb"], 1, old, new)

    for u in range(2):
        for name in STAGES:
            descriptor(u, name).wait_send()


def local(pair_rep, proj_weight, gate_weight, out_weight, in_gain, out_gain):
    turned = jnp.transpose(pair_rep.reshape(128, 2, 16, 128), (3, 1, 2, 0)).reshape(128, 4096)
    vmem = pl.BlockSpec(memory_space=pltpu.VMEM)
    buffers = [
        pltpu.VMEM(shape, BF) for u in range(2) for shape in scratch_of(u).values()
    ]
    result = pl.pallas_call(
        kernel,
        out_shape=jax.ShapeDtypeStruct((128, 4096), BF),
        in_specs=[vmem] * 5 + [pl.BlockSpec(memory_space=pltpu.SMEM)],
        out_specs=vmem,
        scratch_shapes=buffers
        + [
            pltpu.VMEM((2, 6, 128, 128), BF),
            pltpu.VMEM((128, 4096), BF),
            pltpu.VMEM((128, 4096), F32),
            pltpu.VMEM((128, 4096), BF),
            pltpu.VMEM((128 * PITCH, 128), F32),
            pltpu.VMEM((512, 1024), BF),
            pltpu.VMEM((1024, 512), F32),
            pltpu.VMEM((128, 32, 128), BF),
            pltpu.SemaphoreType.DMA((2 * len(STAGES),)),
            pltpu.SemaphoreType.DMA((2 * len(STAGES),)),
        ],
        compiler_params=pltpu.CompilerParams(
            collective_id=0, has_side_effects=True, vmem_limit_bytes=60 * 1024 * 1024
        ),
    )(turned, proj_weight, gate_weight, out_weight, in_gain, out_gain)
    return jnp.transpose(result.reshape(128, 2, 16, 128), (3, 1, 2, 0)).reshape(128, 32, 128)


def solution(mesh):
    placed = (P("row", "col", None), P(), P(), P(), P(), P())
    return jax.shard_map(
        local, mesh=mesh, in_specs=placed, out_specs=P("row", "col", None), check_vma=False
    )
```

```python
import jax
import jax.numpy as jnp
from jax import lax
from jax.experimental import pallas as pl
from jax.experimental.pallas import tpu as pltpu
from jax.sharding import PartitionSpec as P

EPS = 1e-05
MESH = pl.DeviceIdType.MESH
BF = jnp.bfloat16
F32 = jnp.float32
PITCH = 40
LANES = 512

FLOWS = ("first0", "first1", "swap", "last0", "last1", "tri0", "tri1")


def scratch_of(update):
    tile = (16, 128)
    return {
        "first": (128, 2) + tile,
        "last": (128, 2) + tile,
        "all_first": (8, 16, 2, 2) + tile,
        "all_last": ((4, 32, 2) if update == 0 else (8, 16, 2)) + tile,
        "tri": ((2, 4, 32) if update == 0 else (2, 8, 16)) + tile,
        "back": (2, 128) + tile,
    }


NAMES = tuple(scratch_of(0))


def kernel(x_ref, pw_ref, gw_ref, ow_ref, ig_ref, og_ref, out_ref, *scratch):
    count = len(NAMES)
    buffers = [dict(zip(NAMES, scratch[u * count : (u + 1) * count])) for u in range(2)]
    wt, norm, gate, state, stage, right_t, dummy, send_sem, recv_sem = scratch[2 * count :]

    row, col = lax.axis_index("row"), lax.axis_index("col")
    y, xl = lax.div(row, 2), lax.rem(row, 2)
    z, xh, core = lax.div(col, 4), lax.rem(lax.div(col, 2), 2), lax.rem(col, 2)
    x = xh * 2 + xl
    other = 1 - core
    channel = z * 16 + y * 4 + x
    chip_of_col = z * 2 + xh
    side = lax.div(y, 2)
    here_side = side == core

    def device(tx, ty, tz, tc):
        return (ty * 2 + lax.rem(tx, 2), tz * 4 + lax.div(tx, 2) * 2 + tc)

    barrier = pltpu.get_barrier_semaphore()

    @pl.loop(1, 256)
    def _(step):
        there = lax.rem(row * 32 + col + step, 256)
        pl.semaphore_signal(
            barrier, inc=1, device_id=(lax.div(there, 32), lax.rem(there, 32)), device_id_type=MESH
        )

    def copy(update, name, src, dst, target):
        index = update * len(FLOWS) + FLOWS.index(name)
        return pltpu.make_async_remote_copy(
            src_ref=src,
            dst_ref=dst,
            send_sem=send_sem.at[index],
            recv_sem=recv_sem.at[index],
            device_id=target,
            device_id_type=MESH,
        )

    def waits(update, name, kind):
        def wait(tiles):
            whole = dummy.at[pl.ds(0, tiles)]
            handle = copy(update, name, whole, whole, device(x, y, z, other))
            handle.wait_recv() if kind == "recv" else handle.wait_send()

        size = 2 if name.startswith("last") and update == 0 else 1
        if name == "swap":
            wait(256)
        elif update == 0 and not name.startswith("first"):

            @pl.when(here_side)
            def _():
                wait(127 * size)

            @pl.when(jnp.logical_not(here_side))
            def _():
                wait(128 * size)
        else:
            wait(127)

    def arrived(update, name):
        with jax.named_scope(f"wait_{name}_{update}"):
            waits(update, name, "recv")

    def far_first(step, size):
        if isinstance(step, int):
            return (size // 2 + ((step + 1) // 2 if step % 2 else -(step // 2))) % size
        half = lax.div(step + 1, 2)
        away = jnp.where(lax.rem(step, 2) == 1, half, -half)
        return lax.rem(size // 2 + away + size, size)

    def to_chips(one):
        @pl.loop(0, 16)
        def _(step):
            tx = lax.rem(x + far_first(lax.rem(step, 4), 4), 4)
            ty = lax.rem(y + far_first(lax.div(step, 4), 4), 4)
            for k in range(7):
                one(tx, ty, lax.rem(z + far_first(k, 8), 8))

        @pl.loop(0, 15)
        def _(step):
            tx = lax.rem(x + far_first(lax.rem(step, 4), 4), 4)
            ty = lax.rem(y + far_first(lax.div(step, 4), 4), 4)
            one(tx, ty, z)

    def send_same_core(update, name, which, half):
        b = buffers[update]
        landing = b["all_" + which]
        slot = landing.at[row, chip_of_col, core, half] if which == "first" else landing.at[row, chip_of_col, half]

        def one(tx, ty, tz):
            copy(
                update, name, b[which].at[tz * 16 + ty * 4 + tx, half], slot, device(tx, ty, tz, core)
            ).start()

        to_chips(one)
        slot[...] = b[which][channel, half]

    def send_left():
        b = buffers[0]
        slot = b["all_last"].at[lax.rem(row, 4), col]

        def one(tx, ty, tz):
            copy(
                0, "last0", b["last"].at[tz * 16 + ty * 4 + tx], slot, device(tx, ty, tz, side)
            ).start()

        to_chips(one)

        @pl.when(here_side)
        def _():
            slot[...] = b["last"][channel]

        @pl.when(jnp.logical_not(here_side))
        def _():
            one(x, y, z)

    def send_triangle(update, half):
        b = buffers[update]
        name = f"tri{half}"
        slot = b["back"].at[half, channel]
        if update == 1:

            def one(tx, ty, tz):
                src = b["tri"].at[half, ty * 2 + lax.rem(tx, 2), tz * 2 + lax.div(tx, 2)]
                copy(1, name, src, slot, device(tx, ty, tz, core)).start()

            to_chips(one)
            slot[...] = b["tri"][half, row, chip_of_col]
            return

        def one(tx, tq, tz, tc):
            src = b["tri"].at[half, tq * 2 + lax.rem(tx, 2), tz * 4 + lax.div(tx, 2) * 2 + tc]
            copy(0, name, src, slot, device(tx, core * 2 + tq, tz, tc)).start()

        def place(step):
            tx = lax.rem(x + far_first(lax.rem(lax.div(step, 2), 4), 4), 4)
            tq = lax.rem(y + 1 + lax.div(step, 8), 2)
            tc = lax.rem(core + 1 + lax.rem(step, 2), 2)
            return tx, tq, tc

        @pl.loop(0, 16)
        def _(step):
            tx, tq, tc = place(step)
            for k in range(7):
                one(tx, tq, lax.rem(z + far_first(k, 8), 8), tc)

        @pl.loop(0, 15)
        def _(step):
            tx, tq, tc = place(step)
            one(tx, tq, z, tc)

        @pl.when(here_side)
        def _():
            slot[...] = b["tri"][half, lax.rem(row, 4), col]

        @pl.when(jnp.logical_not(here_side))
        def _():
            one(x, lax.rem(y, 2), z, core)

    for u in range(2):
        for p in range(4):
            wt[u, p] = pw_ref[u, p].astype(F32).T.astype(BF)
        wt[u, 4] = gw_ref[u].astype(F32).T.astype(BF)
        wt[u, 5] = ow_ref[u].astype(F32).T.astype(BF)

    tiles = LANES // 128
    per_half = 2048 // LANES

    def lanes(step):
        return pl.ds(pl.multiple_of(step * LANES, LANES), LANES)

    def steps_of(half):
        return pl.loop(half * per_half, (half + 1) * per_half)

    def normalise(update, source, half):
        gain = jnp.broadcast_to(ig_ref[update : update + 1, :], (128, 128)).T
        gain = jnp.concatenate([gain] * tiles, axis=1)

        @steps_of(half)
        def _(step):
            wide = source[:, lanes(step)].astype(F32)
            center = wide - jnp.mean(wide, axis=0, keepdims=True)
            spread = jnp.mean(center * center, axis=0, keepdims=True)
            norm[:, lanes(step)] = (center * lax.rsqrt(spread + EPS) * gain).astype(BF)

    def project(update, hand, target, half):
        weight_gate, weight_value = wt[update, 2 * hand], wt[update, 2 * hand + 1]

        @steps_of(half)
        def _(step):
            normed = norm[:, lanes(step)]
            opening = jnp.dot(weight_gate, normed, preferred_element_type=F32)
            value = jnp.dot(weight_value, normed, preferred_element_type=F32)
            product = jax.nn.sigmoid(opening) * value
            for t in range(tiles):
                stage[pl.ds(step * tiles + t, 128, stride=PITCH), :] = product[:, t * 128 : (t + 1) * 128]

        @pl.loop(0, 8)
        def _(hz):
            for k in range(16):
                start = pl.multiple_of((hz * 16 + k) * PITCH + half * 16, 8)
                target[hz * 16 + k, half] = stage[pl.ds(start, 16), :].astype(BF)

    def gates(update, half):
        weight = wt[update, 4]

        @steps_of(half)
        def _(step):
            opening = jnp.dot(weight, norm[:, lanes(step)], preferred_element_type=F32)
            gate[:, lanes(step)] = jax.nn.sigmoid(opening)

    def turn_right():
        for jb in range(8):
            block = buffers[0]["all_first"][jb].reshape(1024, 128).T.reshape(4, 2, 16, 1024)
            for half in range(2):
                right_t[half, pl.ds(jb * 4, 4)] = block[:, half]

    def contract_outgoing(half):
        b = buffers[0]
        rows = right_t[half].reshape(512, 1024)
        for pair in range(2):
            operand = jnp.concatenate(
                [b["all_last"][pair * 2 + k].reshape(1024, 128) for k in range(2)], axis=1
            )
            product = jnp.dot(rows, operand, preferred_element_type=F32).astype(BF)
            for k in range(2):
                b["tri"][half, pair * 2 + k] = product[:, k * 128 : (k + 1) * 128].reshape(32, 16, 128)

    def contract_incoming(half):
        b = buffers[1]
        rows = jnp.concatenate([b["all_last"][k, :, half].reshape(256, 128) for k in range(8)], axis=1)
        for part in range(4):
            operand = jnp.concatenate(
                [b["all_first"][k, pl.ds(part * 4, 4)].reshape(256, 128) for k in range(8)], axis=1
            )
            product = lax.dot_general(
                rows, operand, (((1,), (1,)), ((), ())), preferred_element_type=F32
            ).astype(BF)
            for k in range(2):
                b["tri"][half, part * 2 + k] = product[:, k * 128 : (k + 1) * 128].reshape(16, 16, 128)

    def finish(update, half, old, new):
        source = buffers[update]["back"]

        def total(read):
            def add(hz, running):
                for k in range(16):
                    running = running + read(hz * 16 + k)
                return running

            return lax.fori_loop(0, 8, add, jnp.zeros((16, 128), F32))

        mean = total(lambda h: source[half, h].astype(F32)) * (1.0 / 128)

        def square(h):
            center = source[half, h].astype(F32) - mean
            return center * center

        inverse = lax.rsqrt(total(square) * (1.0 / 128) + EPS)

        @pl.loop(0, 8)
        def _(hz):
            for k in range(16):
                h = hz * 16 + k
                mixed = (source[half, h].astype(F32) - mean) * inverse * og_ref[update, h]
                stage[pl.ds(pl.multiple_of(h * PITCH, 8), 16), :] = mixed

        weight = wt[update, 5]

        for step in range(per_half):
            mixed = jnp.concatenate(
                [stage[pl.ds(step * tiles + t, 128, stride=PITCH), :] for t in range(tiles)], axis=1
            ).astype(BF)
            change = jnp.dot(weight, mixed, preferred_element_type=F32)
            here = pl.ds(half * 2048 + step * LANES, LANES)
            new[:, here] = (old[:, here].astype(F32) + gate[:, here] * change).astype(BF)

    b = buffers[0]
    for half in range(2):
        normalise(0, x_ref, half)
        project(0, 1, b["first"], half)
        if half == 0:
            with jax.named_scope("barrier"):
                pl.semaphore_wait(barrier, 255)
        with jax.named_scope("send_first"):
            send_same_core(0, f"first{half}", "first", half)
    for half in range(2):
        project(0, 0, b["last"], half)
    with jax.named_scope("send_last"):
        send_left()
    for half in range(2):
        gates(0, half)

    def exchange(update):
        landing = buffers[update]["all_first"]
        for half in range(2):
            arrived(update, f"first{half}")
        own = landing.at[:, :, core]
        copy(update, "swap", own, own, device(x, y, z, other)).start()
        arrived(update, "swap")

    exchange(0)
    with jax.named_scope("turn_right"):
        turn_right()
    arrived(0, "last0")
    for half in range(2):
        with jax.named_scope("contract"):
            contract_outgoing(half)
        with jax.named_scope("send_tri"):
            send_triangle(0, half)

    b = buffers[1]
    for half in range(2):
        arrived(0, f"tri{half}")
        with jax.named_scope("finish"):
            finish(0, half, x_ref, state)
        with jax.named_scope("project"):
            normalise(1, state, half)
            project(1, 0, b["first"], half)
        with jax.named_scope("send_first"):
            send_same_core(1, f"first{half}", "first", half)
    for half in range(2):
        with jax.named_scope("project"):
            project(1, 1, b["last"], half)
        with jax.named_scope("send_last"):
            send_same_core(1, f"last{half}", "last", half)
    for half in range(2):
        gates(1, half)
    exchange(1)
    for half in range(2):
        arrived(1, f"last{half}")
        with jax.named_scope("contract"):
            contract_incoming(half)
        with jax.named_scope("send_tri"):
            send_triangle(1, half)
    for half in range(2):
        arrived(1, f"tri{half}")
        with jax.named_scope("finish"):
            finish(1, half, state, out_ref)

    for u in range(2):
        for name in FLOWS:
            if (u, name) != (0, "last1"):
                waits(u, name, "send")


def local(pair_rep, proj_weight, gate_weight, out_weight, in_gain, out_gain):
    turned = jnp.transpose(pair_rep, (2, 1, 0)).reshape(128, 4096)
    vmem = pl.BlockSpec(memory_space=pltpu.VMEM)
    buffers = [pltpu.VMEM(shape, BF) for u in range(2) for shape in scratch_of(u).values()]
    result = pl.pallas_call(
        kernel,
        out_shape=jax.ShapeDtypeStruct((128, 4096), BF),
        in_specs=[vmem] * 5 + [pl.BlockSpec(memory_space=pltpu.SMEM)],
        out_specs=vmem,
        scratch_shapes=buffers
        + [
            pltpu.VMEM((2, 6, 128, 128), BF),
            pltpu.VMEM((128, 4096), BF),
            pltpu.VMEM((128, 4096), F32),
            pltpu.VMEM((128, 4096), BF),
            pltpu.VMEM((128 * PITCH, 128), F32),
            pltpu.VMEM((2, 32, 16, 1024), BF),
            pltpu.VMEM((256, 16, 128), BF),
            pltpu.SemaphoreType.DMA((2 * len(FLOWS),)),
            pltpu.SemaphoreType.DMA((2 * len(FLOWS),)),
        ],
        compiler_params=pltpu.CompilerParams(
            collective_id=0, has_side_effects=True, vmem_limit_bytes=56 * 1024 * 1024
        ),
    )(turned, proj_weight, gate_weight, out_weight, in_gain, out_gain)
    return jnp.transpose(result.reshape(128, 32, 128), (2, 1, 0))


def solution(mesh):
    placed = (P("row", "col", None), P(), P(), P(), P(), P())
    return jax.shard_map(
        local, mesh=mesh, in_specs=placed, out_specs=P("row", "col", None), check_vma=False
    )
```

```python
import jax
import jax.numpy as jnp
from jax import lax
from jax.experimental import pallas as pl
from jax.experimental.pallas import tpu as pltpu
from jax.sharding import PartitionSpec as P

EPS = 1e-05
MESH = pl.DeviceIdType.MESH
BF = jnp.bfloat16
F32 = jnp.float32
PITCH = 40
LANES = 512

FLOWS = ("first0", "first1", "swap", "last0", "last1", "tri0", "tri1")
FAR_COLS = sorted(range(32), key=lambda c: -min(c, 32 - c))


def scratch_of(update):
    tile = (16, 128)
    return {
        "first": (128, 2) + tile,
        "last": (128, 2) + tile,
        "all_first": (4, 2, 16, 2, 2) + tile,
        "all_last": ((2, 2, 32, 2) if update == 0 else (8, 16, 2)) + tile,
        "tri": ((2, 2, 2, 32) if update == 0 else (2, 8, 16)) + tile,
        "back": (2, 128) + tile,
    }


NAMES = tuple(scratch_of(0))


def kernel(x_in, pw_in, gw_in, ow_in, ig_in, og_in, out_ref, *scratch):
    count = len(NAMES)
    buffers = [dict(zip(NAMES, scratch[u * count : (u + 1) * count])) for u in range(2)]
    (wt, norm, gate, start, state, stage, right_t, dummy, send_sem, recv_sem) = scratch[2 * count : -7]
    x_ref, pw_ref, gw_ref, ow_ref, ig_ref, og_ref, local_sem = scratch[-7:]
    loads = [
        pltpu.make_async_copy(src, dst, local_sem.at[k])
        for k, (src, dst) in enumerate(
            ((x_in, x_ref), (pw_in, pw_ref), (ig_in, ig_ref), (gw_in, gw_ref), (ow_in, ow_ref), (og_in, og_ref))
        )
    ]
    for load in loads:
        load.start()

    row, col = lax.axis_index("row"), lax.axis_index("col")
    y, xl = lax.div(row, 2), lax.rem(row, 2)
    z, xh, core = lax.div(col, 4), lax.rem(lax.div(col, 2), 2), lax.rem(col, 2)
    x = xh * 2 + xl
    other = 1 - core
    channel = z * 16 + y * 4 + x
    chip_of_col = z * 2 + xh
    side = lax.div(y, 2)
    here_side = side == core

    def device(tx, ty, tz, tc):
        return (ty * 2 + lax.rem(tx, 2), tz * 4 + lax.div(tx, 2) * 2 + tc)

    barrier = pltpu.get_barrier_semaphore()

    def greet(to_row, to_col):
        pl.semaphore_signal(barrier, inc=1, device_id=(to_row, to_col), device_id_type=MESH)

    @pl.loop(0, 7)
    def _(step):
        half = lax.div(step + 1, 2)
        to_row = lax.rem(row + 12 + jnp.where(lax.rem(step, 2) == 1, half, -half), 8)
        for away in FAR_COLS:
            greet(to_row, lax.rem(col + away, 32))

    for away in FAR_COLS[:-1]:
        greet(row, lax.rem(col + away, 32))

    def copy(update, name, src, dst, target):
        index = update * len(FLOWS) + FLOWS.index(name)
        return pltpu.make_async_remote_copy(
            src_ref=src,
            dst_ref=dst,
            send_sem=send_sem.at[index],
            recv_sem=recv_sem.at[index],
            device_id=target,
            device_id_type=MESH,
        )

    def waits(update, name, kind):
        def wait(tiles):
            whole = dummy.at[pl.ds(0, tiles)]
            handle = copy(update, name, whole, whole, device(x, y, z, other))
            handle.wait_recv() if kind == "recv" else handle.wait_send()

        def wait_less(tiles, own, less):
            @pl.when(own)
            def _():
                wait(tiles - less)

            @pl.when(jnp.logical_not(own))
            def _():
                wait(tiles)

        if name == "swap":
            wait(256)
        elif update == 0 and not name.startswith("first"):
            wait_less(128, here_side, 1)
        else:
            wait(127)

    def arrived(update, name):
        with jax.named_scope(f"wait_{name}_{update}"):
            waits(update, name, "recv")

    def far_first(step, size):
        if isinstance(step, int):
            return (size // 2 + ((step + 1) // 2 if step % 2 else -(step // 2))) % size
        half = lax.div(step + 1, 2)
        away = jnp.where(lax.rem(step, 2) == 1, half, -half)
        return lax.rem(size // 2 + away + size, size)

    def to_chips(one):
        @pl.loop(0, 16)
        def _(step):
            tx = lax.rem(x + far_first(lax.rem(step, 4), 4), 4)
            ty = lax.rem(y + far_first(lax.div(step, 4), 4), 4)
            for k in range(7):
                one(tx, ty, lax.rem(z + far_first(k, 8), 8))

        @pl.loop(0, 15)
        def _(step):
            tx = lax.rem(x + far_first(lax.rem(step, 4), 4), 4)
            ty = lax.rem(y + far_first(lax.div(step, 4), 4), 4)
            one(tx, ty, z)

    def send_same_core(update, name, which, source, half):
        landing = buffers[update]["all_" + which]
        if which == "first":
            slot = landing.at[y, xl, chip_of_col, core, half]
        else:
            slot = landing.at[row, chip_of_col, half]

        def one(tx, ty, tz):
            copy(
                update, name, source.at[tz * 16 + ty * 4 + tx, half], slot, device(tx, ty, tz, core)
            ).start()

        to_chips(one)
        slot[...] = source[channel, half]

    def send_left(name, source, half):
        slot = buffers[0]["all_last"].at[lax.rem(y, 2), xl, col, half]

        def one(tx, ty, tz):
            copy(
                0, name, source.at[tz * 16 + ty * 4 + tx, half], slot, device(tx, ty, tz, side)
            ).start()

        to_chips(one)

        @pl.when(here_side)
        def _():
            slot[...] = source[channel, half]

        @pl.when(jnp.logical_not(here_side))
        def _():
            one(x, y, z)

    def send_rows(half, yq):
        b = buffers[0]
        slot = b["back"].at[half, channel]

        def one(tx, tz, tc):
            src = b["tri"].at[half, yq, lax.rem(tx, 2), tz * 4 + lax.div(tx, 2) * 2 + tc]
            copy(0, f"tri{half}", src, slot, device(tx, core * 2 + yq, tz, tc)).start()

        def place(step):
            tx = lax.rem(x + far_first(lax.div(step, 2), 4), 4)
            return tx, lax.rem(core + 1 + lax.rem(step, 2), 2)

        @pl.loop(0, 8)
        def _(step):
            tx, tc = place(step)
            for k in range(7):
                one(tx, lax.rem(z + far_first(k, 8), 8), tc)

        for step in range(7):
            tx, tc = place(step)
            one(tx, z, tc)
        own = jnp.logical_and(here_side, lax.rem(y, 2) == yq)

        @pl.when(own)
        def _():
            slot[...] = b["tri"][half, yq, xl, col]

        @pl.when(jnp.logical_not(own))
        def _():
            one(x, z, core)

    def send_triangle(half):
        b = buffers[1]
        slot = b["back"].at[half, channel]

        def one(tx, ty, tz):
            src = b["tri"].at[half, ty * 2 + lax.rem(tx, 2), tz * 2 + lax.div(tx, 2)]
            copy(1, f"tri{half}", src, slot, device(tx, ty, tz, core)).start()

        to_chips(one)
        slot[...] = b["tri"][half, row, chip_of_col]

    def turn_weight(update, index, weight):
        wt[update, index] = weight.astype(F32).T.astype(BF)

    tiles = LANES // 128
    per_half = 2048 // LANES

    def lanes(step):
        return pl.ds(pl.multiple_of(step * LANES, LANES), LANES)

    def steps_of(half):
        return pl.loop(half * per_half, (half + 1) * per_half)

    def load(half):
        rows = pl.ds(half * 16, 16)

        @pl.loop(0, 16)
        def _(step):
            for k in range(8):
                i = step * 8 + k
                stage[pl.ds(pl.multiple_of(i * PITCH + half * 16, 8), 16), :] = x_ref[i, rows, :].astype(F32)

        @steps_of(half)
        def _(step):
            for t in range(tiles):
                block = stage[pl.ds(step * tiles + t, 128, stride=PITCH), :]
                lane = pl.multiple_of(step * LANES + t * 128, 128)
                start[:, pl.ds(lane, 128)] = block.T.astype(BF)

    def normalise(update, source, half):
        gain = jnp.broadcast_to(ig_ref[update : update + 1, :], (128, 128)).T
        gain = jnp.concatenate([gain] * tiles, axis=1)

        @steps_of(half)
        def _(step):
            wide = source[:, lanes(step)].astype(F32)
            center = wide - jnp.mean(wide, axis=0, keepdims=True)
            spread = jnp.mean(center * center, axis=0, keepdims=True)
            norm[:, lanes(step)] = (center * lax.rsqrt(spread + EPS) * gain).astype(BF)

    def project(update, hand, target, half):
        weight_gate, weight_value = wt[update, 2 * hand], wt[update, 2 * hand + 1]

        @steps_of(half)
        def _(step):
            normed = norm[:, lanes(step)]
            opening = jnp.dot(weight_gate, normed, preferred_element_type=F32)
            value = jnp.dot(weight_value, normed, preferred_element_type=F32)
            product = jax.nn.sigmoid(opening) * value
            for t in range(tiles):
                stage[pl.ds(step * tiles + t, 128, stride=PITCH), :] = product[:, t * 128 : (t + 1) * 128]

        @pl.loop(0, 8)
        def _(hz):
            for k in range(16):
                start = pl.multiple_of((hz * 16 + k) * PITCH + half * 16, 8)
                target[hz * 16 + k, half] = stage[pl.ds(start, 16), :].astype(BF)

    def gates(update, half):
        weight = wt[update, 4]

        @steps_of(half)
        def _(step):
            opening = jnp.dot(weight, norm[:, lanes(step)], preferred_element_type=F32)
            gate[:, lanes(step)] = jax.nn.sigmoid(opening)

    def turn_right():
        for jb in range(8):
            block = buffers[0]["all_first"][jb // 2, jb % 2].reshape(1024, 128).T.reshape(4, 2, 16, 1024)
            for half in range(2):
                right_t[half, pl.ds(jb * 4, 4)] = block[:, half]

    def contract_outgoing(half, yq):
        b = buffers[0]
        rows = right_t[half].reshape(512, 1024)
        operand = jnp.concatenate([b["all_last"][yq, k].reshape(1024, 128) for k in range(2)], axis=1)
        product = jnp.dot(rows, operand, preferred_element_type=F32).astype(BF)
        for k in range(2):
            b["tri"][half, yq, k] = product[:, k * 128 : (k + 1) * 128].reshape(32, 16, 128)

    def contract_incoming(half):
        b = buffers[1]
        rows = jnp.concatenate([b["all_last"][k, :, half].reshape(256, 128) for k in range(8)], axis=1)
        for part in range(4):
            operand = jnp.concatenate(
                [
                    b["all_first"][k // 2, k % 2, pl.ds(part * 4, 4)].reshape(256, 128)
                    for k in range(8)
                ],
                axis=1,
            )
            product = lax.dot_general(
                rows, operand, (((1,), (1,)), ((), ())), preferred_element_type=F32
            ).astype(BF)
            for k in range(2):
                b["tri"][half, part * 2 + k] = product[:, k * 128 : (k + 1) * 128].reshape(16, 16, 128)

    def finish(update, half, old):
        source = buffers[update]["back"]

        def total(read):
            def add(hz, running):
                for k in range(16):
                    running = running + read(hz * 16 + k)
                return running

            return lax.fori_loop(0, 8, add, jnp.zeros((16, 128), F32))

        mean = total(lambda h: source[half, h].astype(F32)) * (1.0 / 128)

        def square(h):
            center = source[half, h].astype(F32) - mean
            return center * center

        inverse = lax.rsqrt(total(square) * (1.0 / 128) + EPS)

        @pl.loop(0, 8)
        def _(hz):
            for k in range(16):
                h = hz * 16 + k
                mixed = (source[half, h].astype(F32) - mean) * inverse * og_ref[update, h]
                stage[pl.ds(pl.multiple_of(h * PITCH + half * 16, 8), 16), :] = mixed

        weight = wt[update, 5]

        for step in range(per_half):
            mixed = jnp.concatenate(
                [
                    stage[pl.ds(half * 16 + step * tiles + t, 128, stride=PITCH), :]
                    for t in range(tiles)
                ],
                axis=1,
            ).astype(BF)
            change = jnp.dot(weight, mixed, preferred_element_type=F32)
            here = pl.ds(half * 2048 + step * LANES, LANES)
            total_here = old[:, here].astype(F32) + gate[:, here] * change
            if update == 0:
                state[:, here] = total_here.astype(BF)
                continue
            for t in range(tiles):
                row_of_j = half * 16 + step * tiles + t
                stage[pl.ds(row_of_j, 128, stride=PITCH), :] = total_here[:, t * 128 : (t + 1) * 128].T
        if update == 1:
            rows = pl.ds(half * 16, 16)

            @pl.loop(0, 16)
            def _(step):
                for k in range(8):
                    i = step * 8 + k
                    begin = pl.multiple_of(i * PITCH + half * 16, 8)
                    out_ref[i, rows, :] = stage[pl.ds(begin, 16), :].astype(BF)

    def scope(name, run, *args):
        with jax.named_scope(name):
            run(*args)

    b = buffers[0]
    for k in range(3):
        loads[k].wait()
    for p in range(4):
        turn_weight(0, p, pw_ref[0, p])
    for half in range(2):
        scope("load", load, half)
        scope("normalise", normalise, 0, start, half)
        scope("project", project, 0, 1, b["first"], half)
        if half == 0:
            with jax.named_scope("barrier"):
                pl.semaphore_wait(barrier, 255)
        scope("send_first", send_same_core, 0, f"first{half}", "first", b["first"], half)
    for half in range(2):
        scope("project", project, 0, 0, b["last"], half)
        scope("send_last", send_left, f"last{half}", b["last"], half)
    for k in range(3, 6):
        loads[k].wait()
    for u in range(2):
        if u == 1:
            for p in range(4):
                turn_weight(1, p, pw_ref[1, p])
        turn_weight(u, 4, gw_ref[u])
        turn_weight(u, 5, ow_ref[u])
    for half in range(2):
        scope("gates", gates, 0, half)

    def exchange(update):
        for half in range(2):
            arrived(update, f"first{half}")
        own = buffers[update]["all_first"].at[:, :, :, core]
        copy(update, "swap", own, own, device(x, y, z, other)).start()
        arrived(update, "swap")

    exchange(0)
    scope("turn_right", turn_right)
    for half in range(2):
        arrived(0, f"last{half}")
    for half in range(2):
        for yq in range(2):
            scope("contract", contract_outgoing, half, yq)
            scope("send_tri", send_rows, half, yq)

    b = buffers[1]
    for half in range(2):
        arrived(0, f"tri{half}")
        scope("finish", finish, 0, half, start)
        scope("normalise", normalise, 1, state, half)
        scope("project", project, 1, 0, b["first"], half)
        scope("send_first", send_same_core, 1, f"first{half}", "first", b["first"], half)
    for half in range(2):
        scope("project", project, 1, 1, b["last"], half)
        scope("send_last", send_same_core, 1, f"last{half}", "last", b["last"], half)
    for half in range(2):
        scope("gates", gates, 1, half)
    exchange(1)
    for half in range(2):
        arrived(1, f"last{half}")
        scope("contract", contract_incoming, half)
        scope("send_tri", send_triangle, half)
    for half in range(2):
        arrived(1, f"tri{half}")
        scope("finish", finish, 1, half, state)

    for u in range(2):
        for name in FLOWS:
            waits(u, name, "send")


def local(pair_rep, proj_weight, gate_weight, out_weight, in_gain, out_gain):
    inputs = [
        pltpu.with_memory_space_constraint(array, pltpu.HBM)
        for array in (pair_rep, proj_weight, gate_weight, out_weight, in_gain, out_gain)
    ]
    buffers = [pltpu.VMEM(shape, BF) for u in range(2) for shape in scratch_of(u).values()]
    return pl.pallas_call(
        kernel,
        out_shape=jax.ShapeDtypeStruct((128, 32, 128), BF),
        in_specs=[pl.BlockSpec(memory_space=pltpu.HBM)] * 6,
        out_specs=pl.BlockSpec(memory_space=pltpu.VMEM),
        scratch_shapes=buffers
        + [
            pltpu.VMEM((2, 6, 128, 128), BF),
            pltpu.VMEM((128, 4096), BF),
            pltpu.VMEM((128, 4096), F32),
            pltpu.VMEM((128, 4096), BF),
            pltpu.VMEM((128, 4096), BF),
            pltpu.VMEM((128 * PITCH, 128), F32),
            pltpu.VMEM((2, 32, 16, 1024), BF),
            pltpu.VMEM((256, 16, 128), BF),
            pltpu.SemaphoreType.DMA((2 * len(FLOWS),)),
            pltpu.SemaphoreType.DMA((2 * len(FLOWS),)),
            pltpu.VMEM((128, 32, 128), BF),
            pltpu.VMEM((2, 4, 128, 128), BF),
            pltpu.VMEM((2, 128, 128), BF),
            pltpu.VMEM((2, 128, 128), BF),
            pltpu.VMEM((2, 128), F32),
            pltpu.SMEM((2, 128), F32),
            pltpu.SemaphoreType.DMA((6,)),
        ],
        compiler_params=pltpu.CompilerParams(
            collective_id=0, has_side_effects=True, vmem_limit_bytes=36 * 1024 * 1024
        ),
    )(*inputs)


def solution(mesh):
    placed = (P("row", "col", None), P(), P(), P(), P(), P())
    return jax.shard_map(
        local, mesh=mesh, in_specs=placed, out_specs=P("row", "col", None), check_vma=False
    )
```

```python
import jax
import jax.numpy as jnp
from jax import lax
from jax.experimental import pallas as pl
from jax.experimental.pallas import tpu as pltpu
from jax.sharding import PartitionSpec as P

EPS = 1e-05
MESH = pl.DeviceIdType.MESH
BF = jnp.bfloat16
F32 = jnp.float32
PITCH = 40
LANES = 512

FLOWS = ("first0", "first1", "swap", "last0", "last1", "tri0", "tri1")


def scratch_of(update):
    tile = (16, 128)
    return {
        "first": (128, 2) + tile,
        "last": (128, 2) + tile,
        "all_first": (4, 2, 16, 2, 2) + tile,
        "all_last": ((2, 2, 32, 2) if update == 0 else (8, 16, 2)) + tile,
        "tri": ((2, 2, 2, 32) if update == 0 else (2, 8, 16)) + tile,
        "back": (2, 128) + tile,
    }


NAMES = tuple(scratch_of(0))


def kernel(x_in, pw_in, gw_in, ow_in, ig_in, og_in, out_ref, *scratch):
    count = len(NAMES)
    buffers = [dict(zip(NAMES, scratch[u * count : (u + 1) * count])) for u in range(2)]
    (wt, norm, gate, start, state, stage, right_t, left_n, dummy, send_sem, recv_sem) = scratch[2 * count : -7]
    x_ref, pw_ref, gw_ref, ow_ref, ig_ref, og_ref, local_sem = scratch[-7:]
    loads = [
        pltpu.make_async_copy(src, dst, local_sem.at[k])
        for k, (src, dst) in enumerate(
            ((x_in, x_ref), (pw_in, pw_ref), (ig_in, ig_ref), (gw_in, gw_ref), (ow_in, ow_ref), (og_in, og_ref))
        )
    ]
    for k in range(3):
        loads[k].start()

    row, col = lax.axis_index("row"), lax.axis_index("col")
    y, xl = lax.div(row, 2), lax.rem(row, 2)
    z, xh, core = lax.div(col, 4), lax.rem(lax.div(col, 2), 2), lax.rem(col, 2)
    x = xh * 2 + xl
    other = 1 - core
    channel = z * 16 + y * 4 + x
    chip_of_col = z * 2 + xh
    side = lax.div(y, 2)
    here_side = side == core

    def device(tx, ty, tz, tc):
        return (ty * 2 + lax.rem(tx, 2), tz * 4 + lax.div(tx, 2) * 2 + tc)

    def far_first(step, size):
        if isinstance(step, int):
            return (size // 2 + ((step + 1) // 2 if step % 2 else -(step // 2))) % size
        half = lax.div(step + 1, 2)
        away = jnp.where(lax.rem(step, 2) == 1, half, -half)
        return lax.rem(size // 2 + away + size, size)

    barrier = pltpu.get_barrier_semaphore()

    def greet(to_row, to_col):
        pl.semaphore_signal(barrier, inc=1, device_id=(to_row, to_col), device_id_type=MESH)

    far_rows = [lax.rem(row + away, 8) for away in (4, 3, 5, 2, 6, 1, 7, 0)]

    @pl.loop(0, 31)
    def _(step):
        to_col = lax.rem(col + far_first(step, 32), 32)
        for to_row in far_rows:
            greet(to_row, to_col)

    for to_row in far_rows[:-1]:
        greet(to_row, col)

    for k in range(3, 6):
        loads[k].start()

    def copy(update, name, src, dst, target):
        index = update * len(FLOWS) + FLOWS.index(name)
        return pltpu.make_async_remote_copy(
            src_ref=src,
            dst_ref=dst,
            send_sem=send_sem.at[index],
            recv_sem=recv_sem.at[index],
            device_id=target,
            device_id_type=MESH,
        )

    def waits(update, name, kind):
        def wait(tiles):
            whole = dummy.at[pl.ds(0, tiles)]
            handle = copy(update, name, whole, whole, device(x, y, z, other))
            handle.wait_recv() if kind == "recv" else handle.wait_send()

        def wait_less(tiles, own, less):
            @pl.when(own)
            def _():
                wait(tiles - less)

            @pl.when(jnp.logical_not(own))
            def _():
                wait(tiles)

        if name == "swap":
            wait(256)
        elif update == 0 and not name.startswith("first"):
            wait_less(128, here_side, 1)
        else:
            wait(127)

    def arrived(update, name):
        with jax.named_scope(f"wait_{name}_{update}"):
            waits(update, name, "recv")

    def to_chips(one):
        @pl.loop(0, 16)
        def _(step):
            tx = lax.rem(x + far_first(lax.rem(step, 4), 4), 4)
            ty = lax.rem(y + far_first(lax.div(step, 4), 4), 4)
            for k in range(7):
                one(tx, ty, lax.rem(z + far_first(k, 8), 8))

        @pl.loop(0, 15)
        def _(step):
            tx = lax.rem(x + far_first(lax.rem(step, 4), 4), 4)
            ty = lax.rem(y + far_first(lax.div(step, 4), 4), 4)
            one(tx, ty, z)

    def send_same_core(update, name, which, source, half):
        landing = buffers[update]["all_" + which]
        if which == "first":
            slot = landing.at[y, xl, chip_of_col, core, half]
        else:
            slot = landing.at[row, chip_of_col, half]

        def one(tx, ty, tz):
            copy(
                update, name, source.at[tz * 16 + ty * 4 + tx, half], slot, device(tx, ty, tz, core)
            ).start()

        to_chips(one)
        slot[...] = source[channel, half]

    def send_left(name, source, half):
        slot = buffers[0]["all_last"].at[lax.rem(y, 2), xl, col, half]

        def one(tx, ty, tz):
            copy(
                0, name, source.at[tz * 16 + ty * 4 + tx, half], slot, device(tx, ty, tz, side)
            ).start()

        to_chips(one)

        @pl.when(here_side)
        def _():
            slot[...] = source[channel, half]

        @pl.when(jnp.logical_not(here_side))
        def _():
            one(x, y, z)

    def send_rows(half, yq):
        b = buffers[0]
        slot = b["back"].at[half, channel]

        def one(tx, tz, tc):
            src = b["tri"].at[half, yq, lax.rem(tx, 2), tz * 4 + lax.div(tx, 2) * 2 + tc]
            copy(0, f"tri{half}", src, slot, device(tx, core * 2 + yq, tz, tc)).start()

        def place(step):
            tx = lax.rem(x + far_first(lax.div(step, 2), 4), 4)
            return tx, lax.rem(core + 1 + lax.rem(step, 2), 2)

        @pl.loop(0, 8)
        def _(step):
            tx, tc = place(step)
            for k in range(7):
                one(tx, lax.rem(z + far_first(k, 8), 8), tc)

        for step in range(7):
            tx, tc = place(step)
            one(tx, z, tc)
        own = jnp.logical_and(here_side, lax.rem(y, 2) == yq)

        @pl.when(own)
        def _():
            slot[...] = b["tri"][half, yq, xl, col]

        @pl.when(jnp.logical_not(own))
        def _():
            one(x, z, core)

    def send_triangle(half):
        b = buffers[1]
        slot = b["back"].at[half, channel]

        def one(tx, ty, tz):
            src = b["tri"].at[half, ty * 2 + lax.rem(tx, 2), tz * 2 + lax.div(tx, 2)]
            copy(1, f"tri{half}", src, slot, device(tx, ty, tz, core)).start()

        to_chips(one)
        slot[...] = b["tri"][half, row, chip_of_col]

    def turn_weight(update, index, weight):
        wt[update, index] = weight.astype(F32).T.astype(BF)

    tiles = LANES // 128
    per_half = 2048 // LANES

    def lanes(step):
        return pl.ds(pl.multiple_of(step * LANES, LANES), LANES)

    def steps_of(half):
        return pl.loop(half * per_half, (half + 1) * per_half)

    def halves_of_lanes(first, second):
        return [
            jnp.concatenate([first[..., k : k + 64], second[..., k : k + 64]], axis=-1) for k in (0, 64)
        ]

    def load(half):
        @pl.loop(0, 8)
        def _(step):
            for k in range(8):
                i = half * 64 + step * 8 + k
                stage[pl.ds(pl.multiple_of(i * PITCH, 8), 32), :] = x_ref[i].astype(F32)

        @pl.loop(0, 4)
        def _(step):
            for t in range(4):
                j = step * 4 + t
                block = jnp.concatenate(
                    [
                        stage[pl.ds(half * 64 * PITCH + k * 16 + j, 64, stride=PITCH), :]
                        for k in range(2)
                    ],
                    axis=0,
                )
                lane = pl.multiple_of(half * 2048 + j * 128, 128)
                start[:, pl.ds(lane, 128)] = block.T.astype(BF)

    def unfold():
        for j in range(16):
            tiles_of_j = [state[:, pl.ds((half * 16 + j) * 128, 128)] for half in range(2)]
            for k, tile in enumerate(halves_of_lanes(*tiles_of_j)):
                start[:, pl.ds((k * 16 + j) * 128, 128)] = tile

    def normalise(update, source, half):
        gain = jnp.broadcast_to(ig_ref[update : update + 1, :], (128, 128)).T
        gain = jnp.concatenate([gain] * tiles, axis=1)

        @steps_of(half)
        def _(step):
            wide = source[:, lanes(step)].astype(F32)
            center = wide - jnp.mean(wide, axis=0, keepdims=True)
            spread = jnp.mean(center * center, axis=0, keepdims=True)
            norm[:, lanes(step)] = (center * lax.rsqrt(spread + EPS) * gain).astype(BF)

    def project(update, hand, target, half):
        weight_gate, weight_value = wt[update, 2 * hand], wt[update, 2 * hand + 1]

        @steps_of(half)
        def _(step):
            normed = norm[:, lanes(step)]
            opening = jnp.dot(weight_gate, normed, preferred_element_type=F32)
            value = jnp.dot(weight_value, normed, preferred_element_type=F32)
            product = jax.nn.sigmoid(opening) * value
            for t in range(tiles):
                stage[pl.ds(step * tiles + t, 128, stride=PITCH), :] = product[:, t * 128 : (t + 1) * 128]

        @pl.loop(0, 8)
        def _(hz):
            for k in range(16):
                start = pl.multiple_of((hz * 16 + k) * PITCH + half * 16, 8)
                target[hz * 16 + k, half] = stage[pl.ds(start, 16), :].astype(BF)

    def gates(update, half):
        weight = wt[update, 4]

        @steps_of(half)
        def _(step):
            opening = jnp.dot(weight, norm[:, lanes(step)], preferred_element_type=F32)
            gate[:, lanes(step)] = jax.nn.sigmoid(opening)

    def turn_right():
        for jb in range(8):
            for half in range(2):
                block = buffers[0]["all_first"][jb // 2, jb % 2, :, :, half].reshape(512, 128).T
                for k in range(2):
                    piece = block[k * 64 : (k + 1) * 64].reshape(2, 2, 16, 512)
                    cols = pl.ds(jb * 4 + half * 2, 2)
                    for j_half in range(2):
                        right_t[j_half, cols, :, pl.ds(k * 512, 512)] = piece[:, j_half]

    def turn_left():
        for kb in range(8):
            parts = [buffers[1]["all_first"][kb // 2, kb % 2, :, :, half].reshape(512, 128) for half in range(2)]
            for k, piece in enumerate(halves_of_lanes(*parts)):
                left_n[kb, :, k] = piece.reshape(32, 16, 128)

    def contract_outgoing(half):
        b = buffers[0]
        columns = []
        for yq in range(2):
            parts = [b["all_last"][yq, k, :, half].reshape(512, 128) for k in range(2)]
            columns.append(jnp.concatenate(halves_of_lanes(*parts), axis=0))
        operand = jnp.concatenate(columns, axis=1)
        products = [
            jnp.dot(right_t[k].reshape(512, 1024), operand, preferred_element_type=F32).astype(BF)
            for k in range(2)
        ]
        for yq in range(2):
            parts = [product[:, yq * 128 : (yq + 1) * 128] for product in products]
            for k, piece in enumerate(halves_of_lanes(*parts)):
                b["tri"][half, yq, k] = piece.reshape(32, 16, 128)

    def contract_incoming(half):
        b = buffers[1]
        rows = jnp.concatenate([b["all_last"][k, :, half].reshape(256, 128) for k in range(8)], axis=1)
        for part in range(4):
            operand = jnp.concatenate(
                [
                    left_n[k, pl.ds(part * 8, 8)].reshape(256, 128)
                    for k in range(8)
                ],
                axis=1,
            )
            product = lax.dot_general(
                rows, operand, (((1,), (1,)), ((), ())), preferred_element_type=F32
            ).astype(BF)
            for k in range(2):
                b["tri"][half, part * 2 + k] = product[:, k * 128 : (k + 1) * 128].reshape(16, 16, 128)

    def finish(update, half, old):
        source = buffers[update]["back"]

        def total(read):
            def add(hz, running):
                for k in range(16):
                    running = running + read(hz * 16 + k)
                return running

            return lax.fori_loop(0, 8, add, jnp.zeros((16, 128), F32))

        mean = total(lambda h: source[half, h].astype(F32)) * (1.0 / 128)

        def square(h):
            center = source[half, h].astype(F32) - mean
            return center * center

        inverse = lax.rsqrt(total(square) * (1.0 / 128) + EPS)

        @pl.loop(0, 8)
        def _(hz):
            for k in range(16):
                h = hz * 16 + k
                mixed = (source[half, h].astype(F32) - mean) * inverse * og_ref[update, h]
                stage[pl.ds(pl.multiple_of(h * PITCH + half * 16, 8), 16), :] = mixed

        weight = wt[update, 5]

        for step in range(per_half):
            mixed = jnp.concatenate(
                [
                    stage[pl.ds(half * 16 + step * tiles + t, 128, stride=PITCH), :]
                    for t in range(tiles)
                ],
                axis=1,
            ).astype(BF)
            change = jnp.dot(weight, mixed, preferred_element_type=F32)
            here = pl.ds(half * 2048 + step * LANES, LANES)
            total_here = old[:, here].astype(F32) + gate[:, here] * change
            if update == 0:
                state[:, here] = total_here.astype(BF)
                continue
            for t in range(tiles):
                row_of_j = half * 16 + step * tiles + t
                stage[pl.ds(row_of_j, 128, stride=PITCH), :] = total_here[:, t * 128 : (t + 1) * 128].T
        if update == 1:
            rows = pl.ds(half * 16, 16)

            @pl.loop(0, 16)
            def _(step):
                for k in range(8):
                    i = step * 8 + k
                    begin = pl.multiple_of(i * PITCH + half * 16, 8)
                    out_ref[i, rows, :] = stage[pl.ds(begin, 16), :].astype(BF)

    def scope(name, run, *args):
        with jax.named_scope(name):
            run(*args)

    b = buffers[0]
    for k in range(3):
        loads[k].wait()
    for p in range(4):
        turn_weight(0, p, pw_ref[0, p])
    for half in range(2):
        scope("load", load, half)
        scope("normalise", normalise, 0, start, half)
        scope("project", project, 0, 1, b["first"], half)
        if half == 0:
            with jax.named_scope("barrier"):
                pl.semaphore_wait(barrier, 255)
        scope("send_first", send_same_core, 0, f"first{half}", "first", b["first"], half)
    for half in range(2):
        scope("project", project, 0, 0, b["last"], half)
        scope("send_last", send_left, f"last{half}", b["last"], half)
    for k in range(3, 6):
        loads[k].wait()
    for u in range(2):
        if u == 1:
            for p in range(4):
                turn_weight(1, p, pw_ref[1, p])
        turn_weight(u, 4, gw_ref[u])
        turn_weight(u, 5, ow_ref[u])
    for half in range(2):
        scope("gates", gates, 0, half)

    def exchange(update):
        for half in range(2):
            arrived(update, f"first{half}")
        own = buffers[update]["all_first"].at[:, :, :, core]
        copy(update, "swap", own, own, device(x, y, z, other)).start()
        arrived(update, "swap")

    exchange(0)
    scope("turn_right", turn_right)
    for half in range(2):
        arrived(0, f"last{half}")
        scope("contract", contract_outgoing, half)
        for yq in range(2):
            scope("send_tri", send_rows, half, yq)

    b = buffers[1]
    for half in range(2):
        arrived(0, f"tri{half}")
        scope("finish", finish, 0, half, start)
        scope("normalise", normalise, 1, state, half)
        scope("project", project, 1, 0, b["first"], half)
        scope("send_first", send_same_core, 1, f"first{half}", "first", b["first"], half)
    scope("unfold", unfold)
    for half in range(2):
        scope("normalise", normalise, 1, start, half)
        scope("project", project, 1, 1, b["last"], half)
        scope("send_last", send_same_core, 1, f"last{half}", "last", b["last"], half)
    for half in range(2):
        scope("gates", gates, 1, half)
    exchange(1)
    scope("turn_left", turn_left)
    for half in range(2):
        arrived(1, f"last{half}")
        scope("contract", contract_incoming, half)
        scope("send_tri", send_triangle, half)
    for half in range(2):
        arrived(1, f"tri{half}")
        scope("finish", finish, 1, half, start)

    for u in range(2):
        for name in FLOWS:
            waits(u, name, "send")


def local(pair_rep, proj_weight, gate_weight, out_weight, in_gain, out_gain):
    inputs = [
        pltpu.with_memory_space_constraint(array, pltpu.HBM)
        for array in (pair_rep, proj_weight, gate_weight, out_weight, in_gain, out_gain)
    ]
    buffers = [pltpu.VMEM(shape, BF) for u in range(2) for shape in scratch_of(u).values()]
    return pl.pallas_call(
        kernel,
        out_shape=jax.ShapeDtypeStruct((128, 32, 128), BF),
        in_specs=[pl.BlockSpec(memory_space=pltpu.HBM)] * 6,
        out_specs=pl.BlockSpec(memory_space=pltpu.VMEM),
        scratch_shapes=buffers
        + [
            pltpu.VMEM((2, 6, 128, 128), BF),
            pltpu.VMEM((128, 4096), BF),
            pltpu.VMEM((128, 4096), F32),
            pltpu.VMEM((128, 4096), BF),
            pltpu.VMEM((128, 4096), BF),
            pltpu.VMEM((128 * PITCH, 128), F32),
            pltpu.VMEM((2, 32, 16, 1024), BF),
            pltpu.VMEM((8, 32, 2, 16, 128), BF),
            pltpu.VMEM((256, 16, 128), BF),
            pltpu.SemaphoreType.DMA((2 * len(FLOWS),)),
            pltpu.SemaphoreType.DMA((2 * len(FLOWS),)),
            pltpu.VMEM((128, 32, 128), BF),
            pltpu.VMEM((2, 4, 128, 128), BF),
            pltpu.VMEM((2, 128, 128), BF),
            pltpu.VMEM((2, 128, 128), BF),
            pltpu.VMEM((2, 128), F32),
            pltpu.SMEM((2, 128), F32),
            pltpu.SemaphoreType.DMA((6,)),
        ],
        compiler_params=pltpu.CompilerParams(
            collective_id=0, has_side_effects=True, vmem_limit_bytes=36 * 1024 * 1024
        ),
    )(*inputs)


def solution(mesh):
    placed = (P("row", "col", None), P(), P(), P(), P(), P())
    return jax.shard_map(
        local, mesh=mesh, in_specs=placed, out_specs=P("row", "col", None), check_vma=False
    )
```

```python
import jax
import jax.numpy as jnp
from jax import lax
from jax.experimental import pallas as pl
from jax.experimental.pallas import tpu as pltpu
from jax.sharding import PartitionSpec as P

EPS = 1e-05
MESH = pl.DeviceIdType.MESH
BF = jnp.bfloat16
F32 = jnp.float32
PITCH = 40
LANES = 512

FLOWS = ("first0", "first1", "swap", "last0", "last1", "tri0", "tri1", "pass0", "pass1")
NEAR = ((3, 0), (5, 1), (2, 0), (6, 1), (1, 0), (7, 1))


def scratch_of(update):
    tile = (16, 128)
    return {
        "first": (128, 2) + tile,
        "last": (128, 2) + tile,
        "all_first": ((4, 2, 16, 2, 2) if update == 0 else (2, 4, 2, 8, 2, 2, 2)) + tile,
        "all_last": ((2, 2, 32, 2) if update == 0 else (2, 8, 4, 2, 2)) + tile,
        "tri": ((2, 2, 2, 32) if update == 0 else (2, 2, 8, 4, 2)) + tile,
        "back": (2, 128) + tile,
    }


NAMES = tuple(scratch_of(0))


def kernel(x_in, pw_in, gw_in, ow_in, ig_in, og_in, out_ref, *scratch):
    count = len(NAMES)
    buffers = [dict(zip(NAMES, scratch[u * count : (u + 1) * count])) for u in range(2)]
    (wt, norm, gate, start, state, stage, right_t, left_n, dummy, send_sem, recv_sem) = scratch[2 * count : -7]
    x_ref, pw_ref, gw_ref, ow_ref, ig_ref, og_ref, local_sem = scratch[-7:]
    loads = [
        pltpu.make_async_copy(src, dst, local_sem.at[k])
        for k, (src, dst) in enumerate(
            ((x_in, x_ref), (pw_in, pw_ref), (ig_in, ig_ref), (gw_in, gw_ref), (ow_in, ow_ref), (og_in, og_ref))
        )
    ]
    for k in range(3):
        loads[k].start()

    row, col = lax.axis_index("row"), lax.axis_index("col")
    y, xl = lax.div(row, 2), lax.rem(row, 2)
    z, xh, core = lax.div(col, 4), lax.rem(lax.div(col, 2), 2), lax.rem(col, 2)
    x = xh * 2 + xl
    other = 1 - core
    channel = z * 16 + y * 4 + x
    chip_of_col = z * 2 + xh
    side = lax.div(y, 2)
    here_side = side == core

    def device(tx, ty, tz, tc):
        return (ty * 2 + lax.rem(tx, 2), tz * 4 + lax.div(tx, 2) * 2 + tc)

    def far_first(step, size):
        if isinstance(step, int):
            return (size // 2 + ((step + 1) // 2 if step % 2 else -(step // 2))) % size
        half = lax.div(step + 1, 2)
        away = jnp.where(lax.rem(step, 2) == 1, half, -half)
        return lax.rem(size // 2 + away + size, size)

    barrier = pltpu.get_barrier_semaphore()

    def greet(to_row, to_col):
        pl.semaphore_signal(barrier, inc=1, device_id=(to_row, to_col), device_id_type=MESH)

    far_rows = [lax.rem(row + away, 8) for away in (4, 3, 5, 2, 6, 1, 7, 0)]

    @pl.loop(0, 31)
    def _(step):
        to_col = lax.rem(col + far_first(step, 32), 32)
        for to_row in far_rows:
            greet(to_row, to_col)

    for to_row in far_rows[:-1]:
        greet(to_row, col)

    for k in range(3, 6):
        loads[k].start()

    def copy(update, name, src, dst, target):
        index = update * len(FLOWS) + FLOWS.index(name)
        return pltpu.make_async_remote_copy(
            src_ref=src,
            dst_ref=dst,
            send_sem=send_sem.at[index],
            recv_sem=recv_sem.at[index],
            device_id=target,
            device_id_type=MESH,
        )

    def waits(update, name, kind):
        def wait(tiles):
            whole = dummy.at[pl.ds(0, tiles)]
            handle = copy(update, name, whole, whole, device(x, y, z, other))
            handle.wait_recv() if kind == "recv" else handle.wait_send()

        def wait_less(tiles, own, less):
            @pl.when(own)
            def _():
                wait(tiles - less)

            @pl.when(jnp.logical_not(own))
            def _():
                wait(tiles)

        if name == "swap":
            wait(256 * (update + 1))
        elif update == 1:
            wait(128 if name.startswith("pass") else 126)
        elif name.startswith("first"):
            wait(127)
        else:
            wait_less(128, here_side, 1)

    def arrived(update, name):
        with jax.named_scope(f"wait_{name}_{update}"):
            waits(update, name, "recv")

    def to_chips(one):
        @pl.loop(0, 16)
        def _(step):
            tx = lax.rem(x + far_first(lax.rem(step, 4), 4), 4)
            ty = lax.rem(y + far_first(lax.div(step, 4), 4), 4)
            for k in range(7):
                one(tx, ty, lax.rem(z + far_first(k, 8), 8))

        @pl.loop(0, 15)
        def _(step):
            tx = lax.rem(x + far_first(lax.rem(step, 4), 4), 4)
            ty = lax.rem(y + far_first(lax.div(step, 4), 4), 4)
            one(tx, ty, z)

    def send_right(name, source, half):
        slot = buffers[0]["all_first"].at[y, xl, chip_of_col, core, half]

        def one(tx, ty, tz):
            copy(
                0, name, source.at[tz * 16 + ty * 4 + tx, half], slot, device(tx, ty, tz, core)
            ).start()

        to_chips(one)
        slot[...] = source[channel, half]

    def to_near(one):
        @pl.loop(0, 16)
        def _(step):
            tx = lax.rem(x + far_first(lax.rem(step, 4), 4), 4)
            ty = lax.rem(y + far_first(lax.div(step, 4), 4), 4)
            for hops, role in NEAR:
                one(tx, ty, hops, role)

        @pl.loop(0, 15)
        def _(step):
            tx = lax.rem(x + far_first(lax.rem(step, 4), 4), 4)
            ty = lax.rem(y + far_first(lax.div(step, 4), 4), 4)
            for role in range(2):
                one(tx, ty, 0, role)

    def channel_at(tx, ty, tz, role):
        return lax.rem(tz + 8 - role, 8) * 16 + ty * 4 + tx

    def send_near(which, half):
        b = buffers[1]

        def slot(hops, role):
            if which == "first":
                return b["all_first"].at[role, y, xl, z, xh, core, half]
            return b["all_last"].at[role, row, hops if role == 0 else (8 - hops) % 8, xh, half]

        def one(tx, ty, hops, role):
            tz = lax.rem(z + hops, 8)
            copy(
                1, f"{which}{half}", b[which].at[channel_at(tx, ty, tz, role), half],
                slot(hops, role), device(tx, ty, tz, core),
            ).start()

        to_near(one)
        for role in range(2):
            slot(0, role)[...] = b[which][channel_at(x, y, z, role), half]

    def pass_left(half):
        whole = buffers[1]["all_first"]
        for away in range(4):
            for role in range(2):
                came = lax.rem(z + (8 - away if role == 0 else away), 8)
                to = device(x, y, lax.rem(z + (1 if role == 0 else 7), 8), core)
                src = whole.at[role, :, :, came, :, core, half]
                dst = whole.at[1 - role, :, :, came, :, core, half]
                copy(1, f"pass{half}", src, dst, to).start()

    def send_left(name, source, half):
        slot = buffers[0]["all_last"].at[lax.rem(y, 2), xl, col, half]

        def one(tx, ty, tz):
            copy(
                0, name, source.at[tz * 16 + ty * 4 + tx, half], slot, device(tx, ty, tz, side)
            ).start()

        to_chips(one)

        @pl.when(here_side)
        def _():
            slot[...] = source[channel, half]

        @pl.when(jnp.logical_not(here_side))
        def _():
            one(x, y, z)

    def send_rows(half, yq):
        b = buffers[0]
        slot = b["back"].at[half, channel]

        def one(tx, tz, tc):
            src = b["tri"].at[half, yq, lax.rem(tx, 2), tz * 4 + lax.div(tx, 2) * 2 + tc]
            copy(0, f"tri{half}", src, slot, device(tx, core * 2 + yq, tz, tc)).start()

        def place(step):
            tx = lax.rem(x + far_first(lax.div(step, 2), 4), 4)
            return tx, lax.rem(core + 1 + lax.rem(step, 2), 2)

        @pl.loop(0, 8)
        def _(step):
            tx, tc = place(step)
            for k in range(7):
                one(tx, lax.rem(z + far_first(k, 8), 8), tc)

        for step in range(7):
            tx, tc = place(step)
            one(tx, z, tc)
        own = jnp.logical_and(here_side, lax.rem(y, 2) == yq)

        @pl.when(own)
        def _():
            slot[...] = b["tri"][half, yq, xl, col]

        @pl.when(jnp.logical_not(own))
        def _():
            one(x, z, core)

    def send_triangle(half):
        b = buffers[1]

        def slot(role):
            return b["back"].at[half, channel_at(x, y, z, role)]

        def one(tx, ty, hops, role):
            away = hops if role == 0 else (8 - hops) % 8
            src = b["tri"].at[half, role, ty * 2 + lax.rem(tx, 2), away, lax.div(tx, 2)]
            target = device(tx, ty, lax.rem(z + 8 - hops, 8), core)
            copy(1, f"tri{half}", src, slot(role), target).start()

        to_near(one)
        for role in range(2):
            slot(role)[...] = b["tri"][half, role, row, 0, xh]

    def turn_weight(update, index, weight):
        wt[update, index] = weight.astype(F32).T.astype(BF)

    tiles = LANES // 128
    per_half = 2048 // LANES

    def lanes(step):
        return pl.ds(pl.multiple_of(step * LANES, LANES), LANES)

    def steps_of(half):
        return pl.loop(half * per_half, (half + 1) * per_half)

    def halves_of_lanes(first, second):
        return [
            jnp.concatenate([first[..., k : k + 64], second[..., k : k + 64]], axis=-1) for k in (0, 64)
        ]

    def load(half):
        @pl.loop(0, 8)
        def _(step):
            for k in range(8):
                i = half * 64 + step * 8 + k
                stage[pl.ds(pl.multiple_of(i * PITCH, 8), 32), :] = x_ref[i].astype(F32)

        @pl.loop(0, 4)
        def _(step):
            for t in range(4):
                j = step * 4 + t
                block = jnp.concatenate(
                    [
                        stage[pl.ds(half * 64 * PITCH + k * 16 + j, 64, stride=PITCH), :]
                        for k in range(2)
                    ],
                    axis=0,
                )
                lane = pl.multiple_of(half * 2048 + j * 128, 128)
                start[:, pl.ds(lane, 128)] = block.T.astype(BF)

    def unfold():
        for j in range(16):
            tiles_of_j = [state[:, pl.ds((half * 16 + j) * 128, 128)] for half in range(2)]
            for k, tile in enumerate(halves_of_lanes(*tiles_of_j)):
                start[:, pl.ds((k * 16 + j) * 128, 128)] = tile

    def normalise(update, source, half):
        gain = jnp.broadcast_to(ig_ref[update : update + 1, :], (128, 128)).T
        gain = jnp.concatenate([gain] * tiles, axis=1)

        @steps_of(half)
        def _(step):
            wide = source[:, lanes(step)].astype(F32)
            center = wide - jnp.mean(wide, axis=0, keepdims=True)
            spread = jnp.mean(center * center, axis=0, keepdims=True)
            norm[:, lanes(step)] = (center * lax.rsqrt(spread + EPS) * gain).astype(BF)

    def project(update, hand, target, half):
        weight_gate, weight_value = wt[update, 2 * hand], wt[update, 2 * hand + 1]

        @steps_of(half)
        def _(step):
            normed = norm[:, lanes(step)]
            opening = jnp.dot(weight_gate, normed, preferred_element_type=F32)
            value = jnp.dot(weight_value, normed, preferred_element_type=F32)
            product = jax.nn.sigmoid(opening) * value
            for t in range(tiles):
                stage[pl.ds(step * tiles + t, 128, stride=PITCH), :] = product[:, t * 128 : (t + 1) * 128]

        @pl.loop(0, 8)
        def _(hz):
            for k in range(16):
                start = pl.multiple_of((hz * 16 + k) * PITCH + half * 16, 8)
                target[hz * 16 + k, half] = stage[pl.ds(start, 16), :].astype(BF)

    def gates(update, half):
        weight = wt[update, 4]

        @steps_of(half)
        def _(step):
            opening = jnp.dot(weight, norm[:, lanes(step)], preferred_element_type=F32)
            gate[:, lanes(step)] = jax.nn.sigmoid(opening)

    def turn_right():
        for jb in range(8):
            for half in range(2):
                block = buffers[0]["all_first"][jb // 2, jb % 2, :, :, half].reshape(512, 128).T
                for k in range(2):
                    piece = block[k * 64 : (k + 1) * 64].reshape(2, 2, 16, 512)
                    cols = pl.ds(jb * 4 + half * 2, 2)
                    for j_half in range(2):
                        right_t[j_half, cols, :, pl.ds(k * 512, 512)] = piece[:, j_half]

    def turn_left():
        for role in range(2):
            for kb in range(8):
                whole = buffers[1]["all_first"]
                parts = [whole[role, kb // 2, kb % 2, :, :, :, half].reshape(512, 128) for half in range(2)]
                for k, piece in enumerate(halves_of_lanes(*parts)):
                    left_n[role, kb, :, k] = piece.reshape(32, 16, 128)

    def contract_outgoing(half):
        b = buffers[0]
        columns = []
        for yq in range(2):
            parts = [b["all_last"][yq, k, :, half].reshape(512, 128) for k in range(2)]
            columns.append(jnp.concatenate(halves_of_lanes(*parts), axis=0))
        operand = jnp.concatenate(columns, axis=1)
        products = [
            jnp.dot(right_t[k].reshape(512, 1024), operand, preferred_element_type=F32).astype(BF)
            for k in range(2)
        ]
        for yq in range(2):
            parts = [product[:, yq * 128 : (yq + 1) * 128] for product in products]
            for k, piece in enumerate(halves_of_lanes(*parts)):
                b["tri"][half, yq, k] = piece.reshape(32, 16, 128)

    def contract_incoming(half):
        b = buffers[1]
        for role in range(2):
            rows = jnp.concatenate(
                [b["all_last"][role, k, :, :, half].reshape(128, 128) for k in range(8)], axis=1
            )
            for part in range(4):
                operand = jnp.concatenate(
                    [left_n[role, k, pl.ds(part * 8, 8)].reshape(256, 128) for k in range(8)], axis=1
                )
                product = lax.dot_general(
                    rows, operand, (((1,), (1,)), ((), ())), preferred_element_type=F32
                ).astype(BF)
                for k in range(2):
                    piece = product[:, k * 128 : (k + 1) * 128].reshape(4, 2, 16, 128)
                    b["tri"][half, role, part * 2 + k] = piece

    def finish(update, half, old):
        source = buffers[update]["back"]

        def total(read):
            def add(hz, running):
                for k in range(16):
                    running = running + read(hz * 16 + k)
                return running

            return lax.fori_loop(0, 8, add, jnp.zeros((16, 128), F32))

        mean = total(lambda h: source[half, h].astype(F32)) * (1.0 / 128)

        def square(h):
            center = source[half, h].astype(F32) - mean
            return center * center

        inverse = lax.rsqrt(total(square) * (1.0 / 128) + EPS)

        @pl.loop(0, 8)
        def _(hz):
            for k in range(16):
                h = hz * 16 + k
                mixed = (source[half, h].astype(F32) - mean) * inverse * og_ref[update, h]
                stage[pl.ds(pl.multiple_of(h * PITCH + half * 16, 8), 16), :] = mixed

        weight = wt[update, 5]

        for step in range(per_half):
            mixed = jnp.concatenate(
                [
                    stage[pl.ds(half * 16 + step * tiles + t, 128, stride=PITCH), :]
                    for t in range(tiles)
                ],
                axis=1,
            ).astype(BF)
            change = jnp.dot(weight, mixed, preferred_element_type=F32)
            here = pl.ds(half * 2048 + step * LANES, LANES)
            total_here = old[:, here].astype(F32) + gate[:, here] * change
            if update == 0:
                state[:, here] = total_here.astype(BF)
                continue
            for t in range(tiles):
                row_of_j = half * 16 + step * tiles + t
                stage[pl.ds(row_of_j, 128, stride=PITCH), :] = total_here[:, t * 128 : (t + 1) * 128].T
        if update == 1:
            rows = pl.ds(half * 16, 16)

            @pl.loop(0, 16)
            def _(step):
                for k in range(8):
                    i = step * 8 + k
                    begin = pl.multiple_of(i * PITCH + half * 16, 8)
                    out_ref[i, rows, :] = stage[pl.ds(begin, 16), :].astype(BF)

    def scope(name, run, *args):
        with jax.named_scope(name):
            run(*args)

    b = buffers[0]
    for k in range(3):
        loads[k].wait()
    for p in range(4):
        turn_weight(0, p, pw_ref[0, p])
    for half in range(2):
        scope("load", load, half)
        scope("normalise", normalise, 0, start, half)
        scope("project", project, 0, 1, b["first"], half)
        if half == 0:
            with jax.named_scope("barrier"):
                pl.semaphore_wait(barrier, 255)
        scope("send_first", send_right, f"first{half}", b["first"], half)
    for half in range(2):
        scope("project", project, 0, 0, b["last"], half)
        scope("send_last", send_left, f"last{half}", b["last"], half)
    for k in range(3, 6):
        loads[k].wait()
    for u in range(2):
        if u == 1:
            for p in range(4):
                turn_weight(1, p, pw_ref[1, p])
        turn_weight(u, 4, gw_ref[u])
        turn_weight(u, 5, ow_ref[u])
    for half in range(2):
        scope("gates", gates, 0, half)

    def swap(update):
        whole = buffers[update]["all_first"]
        own = whole.at[:, :, :, core] if update == 0 else whole.at[:, :, :, :, :, core]
        copy(update, "swap", own, own, device(x, y, z, other)).start()
        arrived(update, "swap")

    for half in range(2):
        arrived(0, f"first{half}")
    swap(0)
    scope("turn_right", turn_right)
    for half in range(2):
        arrived(0, f"last{half}")
        scope("contract", contract_outgoing, half)
        for yq in range(2):
            scope("send_tri", send_rows, half, yq)

    b = buffers[1]
    for half in range(2):
        arrived(0, f"tri{half}")
        scope("finish", finish, 0, half, start)
        scope("normalise", normalise, 1, state, half)
        scope("project", project, 1, 0, b["first"], half)
        scope("send_first", send_near, "first", half)
    scope("unfold", unfold)
    for half in range(2):
        scope("normalise", normalise, 1, start, half)
        scope("project", project, 1, 1, b["last"], half)
    for half in range(2):
        scope("gates", gates, 1, half)
    for half in range(2):
        arrived(1, f"first{half}")
        scope("pass", pass_left, half)
    for half in range(2):
        scope("send_last", send_near, "last", half)
    for half in range(2):
        arrived(1, f"pass{half}")
    swap(1)
    scope("turn_left", turn_left)
    for half in range(2):
        arrived(1, f"last{half}")
        scope("contract", contract_incoming, half)
        scope("send_tri", send_triangle, half)
    for half in range(2):
        arrived(1, f"tri{half}")
        scope("finish", finish, 1, half, start)

    for u in range(2):
        for name in FLOWS:
            if u == 1 or not name.startswith("pass"):
                waits(u, name, "send")


def local(pair_rep, proj_weight, gate_weight, out_weight, in_gain, out_gain):
    inputs = [
        pltpu.with_memory_space_constraint(array, pltpu.HBM)
        for array in (pair_rep, proj_weight, gate_weight, out_weight, in_gain, out_gain)
    ]
    buffers = [pltpu.VMEM(shape, BF) for u in range(2) for shape in scratch_of(u).values()]
    return pl.pallas_call(
        kernel,
        out_shape=jax.ShapeDtypeStruct((128, 32, 128), BF),
        in_specs=[pl.BlockSpec(memory_space=pltpu.HBM)] * 6,
        out_specs=pl.BlockSpec(memory_space=pltpu.VMEM),
        scratch_shapes=buffers
        + [
            pltpu.VMEM((2, 6, 128, 128), BF),
            pltpu.VMEM((128, 4096), BF),
            pltpu.VMEM((128, 4096), F32),
            pltpu.VMEM((128, 4096), BF),
            pltpu.VMEM((128, 4096), BF),
            pltpu.VMEM((128 * PITCH, 128), F32),
            pltpu.VMEM((2, 32, 16, 1024), BF),
            pltpu.VMEM((2, 8, 32, 2, 16, 128), BF),
            pltpu.VMEM((512, 16, 128), BF),
            pltpu.SemaphoreType.DMA((2 * len(FLOWS),)),
            pltpu.SemaphoreType.DMA((2 * len(FLOWS),)),
            pltpu.VMEM((128, 32, 128), BF),
            pltpu.VMEM((2, 4, 128, 128), BF),
            pltpu.VMEM((2, 128, 128), BF),
            pltpu.VMEM((2, 128, 128), BF),
            pltpu.VMEM((2, 128), F32),
            pltpu.SMEM((2, 128), F32),
            pltpu.SemaphoreType.DMA((6,)),
        ],
        compiler_params=pltpu.CompilerParams(
            collective_id=0, has_side_effects=True, vmem_limit_bytes=44 * 1024 * 1024
        ),
    )(*inputs)


def solution(mesh):
    placed = (P("row", "col", None), P(), P(), P(), P(), P())
    return jax.shard_map(
        local, mesh=mesh, in_specs=placed, out_specs=P("row", "col", None), check_vma=False
    )
```

```python
import jax
import jax.numpy as jnp
from jax import lax
from jax.experimental import pallas as pl
from jax.experimental.pallas import tpu as pltpu
from jax.sharding import PartitionSpec as P

EPS = 1e-05
MESH = pl.DeviceIdType.MESH
BF = jnp.bfloat16
F32 = jnp.float32
PITCH = 40
LANES = 512

FLOWS = ("first0", "first1", "swap", "last0", "last1", "tri0", "tri1", "pass0", "pass1")
NEAR = ((3, 0), (5, 1), (2, 0), (6, 1), (1, 0), (7, 1))


def scratch_of(update):
    tile = (16, 128)
    return {
        "first": (128, 2) + tile,
        "last": (128, 2) + tile,
        "all_first": ((4, 2, 16, 2, 2) if update == 0 else (2, 4, 2, 8, 2, 2, 2)) + tile,
        "all_last": ((2, 2, 32, 2) if update == 0 else (2, 8, 4, 2, 2)) + tile,
        "tri": ((2, 2, 2, 32) if update == 0 else (2, 2, 8, 4, 2)) + tile,
        "back": (2, 128) + tile,
    }


NAMES = tuple(scratch_of(0))


def kernel(x_in, pw_in, gw_in, ow_in, ig_in, og_in, out_ref, *scratch):
    count = len(NAMES)
    buffers = [dict(zip(NAMES, scratch[u * count : (u + 1) * count])) for u in range(2)]
    (wt, norm, gate, start, state, stage, right_t, left_n, dummy, send_sem, recv_sem) = scratch[2 * count : -7]
    x_ref, pw_ref, gw_ref, ow_ref, ig_ref, og_ref, local_sem = scratch[-7:]
    loads = [
        pltpu.make_async_copy(src, dst, local_sem.at[k])
        for k, (src, dst) in enumerate(
            ((x_in, x_ref), (pw_in, pw_ref), (ig_in, ig_ref), (gw_in, gw_ref), (ow_in, ow_ref), (og_in, og_ref))
        )
    ]
    for k in range(3):
        loads[k].start()

    row, col = lax.axis_index("row"), lax.axis_index("col")
    y, xl = lax.div(row, 2), lax.rem(row, 2)
    z, xh, core = lax.div(col, 4), lax.rem(lax.div(col, 2), 2), lax.rem(col, 2)
    x = xh * 2 + xl
    other = 1 - core
    channel = z * 16 + y * 4 + x
    chip_of_col = z * 2 + xh
    side = lax.div(y, 2)
    here_side = side == core

    def device(tx, ty, tz, tc):
        return (ty * 2 + lax.rem(tx, 2), tz * 4 + lax.div(tx, 2) * 2 + tc)

    def far_first(step, size):
        if isinstance(step, int):
            return (size // 2 + ((step + 1) // 2 if step % 2 else -(step // 2))) % size
        half = lax.div(step + 1, 2)
        away = jnp.where(lax.rem(step, 2) == 1, half, -half)
        return lax.rem(size // 2 + away + size, size)

    barrier = pltpu.get_barrier_semaphore()

    def greet(to_row, to_col):
        pl.semaphore_signal(barrier, inc=1, device_id=(to_row, to_col), device_id_type=MESH)

    far_rows = [lax.rem(row + away, 8) for away in (4, 3, 5, 2, 6, 1, 7, 0)]

    @pl.loop(0, 31)
    def _(step):
        to_col = lax.rem(col + far_first(step, 32), 32)
        for to_row in far_rows:
            greet(to_row, to_col)

    for to_row in far_rows[:-1]:
        greet(to_row, col)

    for k in range(3, 6):
        loads[k].start()

    def copy(update, name, src, dst, target):
        index = update * len(FLOWS) + FLOWS.index(name)
        return pltpu.make_async_remote_copy(
            src_ref=src,
            dst_ref=dst,
            send_sem=send_sem.at[index],
            recv_sem=recv_sem.at[index],
            device_id=target,
            device_id_type=MESH,
        )

    def waits(update, name, kind):
        def wait(tiles):
            whole = dummy.at[pl.ds(0, tiles)]
            handle = copy(update, name, whole, whole, device(x, y, z, other))
            handle.wait_recv() if kind == "recv" else handle.wait_send()

        def wait_less(tiles, own, less):
            @pl.when(own)
            def _():
                wait(tiles - less)

            @pl.when(jnp.logical_not(own))
            def _():
                wait(tiles)

        if name == "swap":
            wait(256 * (update + 1))
        elif update == 1:
            wait(128 if name.startswith("pass") else 126)
        elif name.startswith("first"):
            wait(127)
        else:
            wait_less(128, here_side, 1)

    def arrived(update, name):
        with jax.named_scope(f"wait_{name}_{update}"):
            waits(update, name, "recv")

    def to_chips(one):
        @pl.loop(0, 16)
        def _(step):
            tx = lax.rem(x + far_first(lax.rem(step, 4), 4), 4)
            ty = lax.rem(y + far_first(lax.div(step, 4), 4), 4)
            for k in range(7):
                one(tx, ty, lax.rem(z + far_first(k, 8), 8))

        @pl.loop(0, 15)
        def _(step):
            tx = lax.rem(x + far_first(lax.rem(step, 4), 4), 4)
            ty = lax.rem(y + far_first(lax.div(step, 4), 4), 4)
            one(tx, ty, z)

    def send_right(name, source, half):
        slot = buffers[0]["all_first"].at[y, xl, chip_of_col, core, half]

        def one(tx, ty, tz):
            copy(
                0, name, source.at[tz * 16 + ty * 4 + tx, half], slot, device(tx, ty, tz, core)
            ).start()

        to_chips(one)
        slot[...] = source[channel, half]

    def to_near(one):
        @pl.loop(0, 16)
        def _(step):
            tx = lax.rem(x + far_first(lax.rem(step, 4), 4), 4)
            ty = lax.rem(y + far_first(lax.div(step, 4), 4), 4)
            for hops, role in NEAR:
                one(tx, ty, hops, role)

        @pl.loop(0, 15)
        def _(step):
            tx = lax.rem(x + far_first(lax.rem(step, 4), 4), 4)
            ty = lax.rem(y + far_first(lax.div(step, 4), 4), 4)
            for role in range(2):
                one(tx, ty, 0, role)

    def channel_at(tx, ty, tz, role):
        return lax.rem(tz + 8 - role, 8) * 16 + ty * 4 + tx

    def send_near(which, half):
        b = buffers[1]

        def slot(hops, role):
            if which == "first":
                return b["all_first"].at[role, y, xl, z, xh, core, half]
            return b["all_last"].at[role, row, hops if role == 0 else (8 - hops) % 8, xh, half]

        def one(tx, ty, hops, role):
            tz = lax.rem(z + hops, 8)
            copy(
                1, f"{which}{half}", b[which].at[channel_at(tx, ty, tz, role), half],
                slot(hops, role), device(tx, ty, tz, core),
            ).start()

        to_near(one)
        for role in range(2):
            slot(0, role)[...] = b[which][channel_at(x, y, z, role), half]

    def pass_left(half):
        whole = buffers[1]["all_first"]
        for away in range(4):
            for role in range(2):
                came = lax.rem(z + (8 - away if role == 0 else away), 8)
                to = device(x, y, lax.rem(z + (1 if role == 0 else 7), 8), core)
                src = whole.at[role, :, :, came, :, core, half]
                dst = whole.at[1 - role, :, :, came, :, core, half]
                copy(1, f"pass{half}", src, dst, to).start()

    def send_left(name, source, half):
        slot = buffers[0]["all_last"].at[lax.rem(y, 2), xl, col, half]

        def one(tx, ty, tz):
            copy(
                0, name, source.at[tz * 16 + ty * 4 + tx, half], slot, device(tx, ty, tz, side)
            ).start()

        to_chips(one)

        @pl.when(here_side)
        def _():
            slot[...] = source[channel, half]

        @pl.when(jnp.logical_not(here_side))
        def _():
            one(x, y, z)

    def send_rows(half, yq):
        b = buffers[0]
        slot = b["back"].at[half, channel]

        def one(tx, tz, tc):
            src = b["tri"].at[half, yq, lax.rem(tx, 2), tz * 4 + lax.div(tx, 2) * 2 + tc]
            copy(0, f"tri{half}", src, slot, device(tx, core * 2 + yq, tz, tc)).start()

        def place(step):
            tx = lax.rem(x + far_first(lax.div(step, 2), 4), 4)
            return tx, lax.rem(core + 1 + lax.rem(step, 2), 2)

        @pl.loop(0, 8)
        def _(step):
            tx, tc = place(step)
            for k in range(7):
                one(tx, lax.rem(z + far_first(k, 8), 8), tc)

        for step in range(7):
            tx, tc = place(step)
            one(tx, z, tc)
        own = jnp.logical_and(here_side, lax.rem(y, 2) == yq)

        @pl.when(own)
        def _():
            slot[...] = b["tri"][half, yq, xl, col]

        @pl.when(jnp.logical_not(own))
        def _():
            one(x, z, core)

    def send_triangle(half, step):
        b = buffers[1]
        ty = lax.rem(y + far_first(step, 4), 4)
        contract_incoming(half, ty)

        def slot(role):
            return b["back"].at[half, channel_at(x, y, z, role)]

        def one(tx, hops, role):
            away = hops if role == 0 else (8 - hops) % 8
            src = b["tri"].at[half, role, ty * 2 + lax.rem(tx, 2), away, lax.div(tx, 2)]
            target = device(tx, ty, lax.rem(z + 8 - hops, 8), core)
            copy(1, f"tri{half}", src, slot(role), target).start()

        for k in range(4):
            for hops, role in NEAR:
                one(lax.rem(x + far_first(k, 4), 4), hops, role)
        for k in range(3 if step == 3 else 4):
            for role in range(2):
                one(lax.rem(x + far_first(k, 4), 4), 0, role)
        if step == 3:
            for role in range(2):
                slot(role)[...] = b["tri"][half, role, row, 0, xh]

    def turn_weight(update, index, weight):
        wt[update, index] = weight.astype(F32).T.astype(BF)

    tiles = LANES // 128
    per_half = 2048 // LANES

    def lanes(step):
        return pl.ds(pl.multiple_of(step * LANES, LANES), LANES)

    def steps_of(half):
        return pl.loop(half * per_half, (half + 1) * per_half)

    def halves_of_lanes(first, second):
        return [
            jnp.concatenate([first[..., k : k + 64], second[..., k : k + 64]], axis=-1) for k in (0, 64)
        ]

    def load(half):
        @pl.loop(0, 8)
        def _(step):
            for k in range(8):
                i = half * 64 + step * 8 + k
                stage[pl.ds(pl.multiple_of(i * PITCH, 8), 32), :] = x_ref[i].astype(F32)

        @pl.loop(0, 4)
        def _(step):
            for t in range(4):
                j = step * 4 + t
                block = jnp.concatenate(
                    [
                        stage[pl.ds(half * 64 * PITCH + k * 16 + j, 64, stride=PITCH), :]
                        for k in range(2)
                    ],
                    axis=0,
                )
                lane = pl.multiple_of(half * 2048 + j * 128, 128)
                start[:, pl.ds(lane, 128)] = block.T.astype(BF)

    def unfold():
        for j in range(16):
            tiles_of_j = [state[:, pl.ds((half * 16 + j) * 128, 128)] for half in range(2)]
            for k, tile in enumerate(halves_of_lanes(*tiles_of_j)):
                start[:, pl.ds((k * 16 + j) * 128, 128)] = tile

    def normalise(update, source, half):
        gain = jnp.broadcast_to(ig_ref[update : update + 1, :], (128, 128)).T
        gain = jnp.concatenate([gain] * tiles, axis=1)

        @steps_of(half)
        def _(step):
            wide = source[:, lanes(step)].astype(F32)
            center = wide - jnp.mean(wide, axis=0, keepdims=True)
            spread = jnp.mean(center * center, axis=0, keepdims=True)
            norm[:, lanes(step)] = (center * lax.rsqrt(spread + EPS) * gain).astype(BF)

    def project(update, hand, target, half):
        weight_gate, weight_value = wt[update, 2 * hand], wt[update, 2 * hand + 1]

        @steps_of(half)
        def _(step):
            normed = norm[:, lanes(step)]
            opening = jnp.dot(weight_gate, normed, preferred_element_type=F32)
            value = jnp.dot(weight_value, normed, preferred_element_type=F32)
            product = jax.nn.sigmoid(opening) * value
            for t in range(tiles):
                stage[pl.ds(step * tiles + t, 128, stride=PITCH), :] = product[:, t * 128 : (t + 1) * 128]

        @pl.loop(0, 8)
        def _(hz):
            for k in range(16):
                start = pl.multiple_of((hz * 16 + k) * PITCH + half * 16, 8)
                target[hz * 16 + k, half] = stage[pl.ds(start, 16), :].astype(BF)

    def gates(update, half):
        weight = wt[update, 4]

        @steps_of(half)
        def _(step):
            opening = jnp.dot(weight, norm[:, lanes(step)], preferred_element_type=F32)
            gate[:, lanes(step)] = jax.nn.sigmoid(opening)

    def turn_right():
        for jb in range(8):
            for half in range(2):
                block = buffers[0]["all_first"][jb // 2, jb % 2, :, :, half].reshape(512, 128).T
                for k in range(2):
                    piece = block[k * 64 : (k + 1) * 64].reshape(2, 2, 16, 512)
                    cols = pl.ds(jb * 4 + half * 2, 2)
                    for j_half in range(2):
                        right_t[j_half, cols, :, pl.ds(k * 512, 512)] = piece[:, j_half]

    def turn_left():
        for role in range(2):
            for kb in range(8):
                whole = buffers[1]["all_first"]
                parts = [whole[role, kb // 2, kb % 2, :, :, :, half].reshape(512, 128) for half in range(2)]
                for k, piece in enumerate(halves_of_lanes(*parts)):
                    left_n[role, kb, :, k] = piece.reshape(32, 16, 128)

    def contract_outgoing(half):
        b = buffers[0]
        columns = []
        for yq in range(2):
            parts = [b["all_last"][yq, k, :, half].reshape(512, 128) for k in range(2)]
            columns.append(jnp.concatenate(halves_of_lanes(*parts), axis=0))
        operand = jnp.concatenate(columns, axis=1)
        products = [
            jnp.dot(right_t[k].reshape(512, 1024), operand, preferred_element_type=F32).astype(BF)
            for k in range(2)
        ]
        for yq in range(2):
            parts = [product[:, yq * 128 : (yq + 1) * 128] for product in products]
            for k, piece in enumerate(halves_of_lanes(*parts)):
                b["tri"][half, yq, k] = piece.reshape(32, 16, 128)

    def contract_incoming(half, part):
        b = buffers[1]
        for role in range(2):
            rows = jnp.concatenate(
                [b["all_last"][role, k, :, :, half].reshape(128, 128) for k in range(8)], axis=1
            )
            operand = jnp.concatenate(
                [left_n[role, k, pl.ds(part * 8, 8)].reshape(256, 128) for k in range(8)], axis=1
            )
            product = lax.dot_general(
                rows, operand, (((1,), (1,)), ((), ())), preferred_element_type=F32
            ).astype(BF)
            for k in range(2):
                piece = product[:, k * 128 : (k + 1) * 128].reshape(4, 2, 16, 128)
                b["tri"][half, role, part * 2 + k] = piece

    def finish(update, half, old):
        source = buffers[update]["back"]

        def total(read):
            def add(hz, running):
                for k in range(16):
                    running = running + read(hz * 16 + k)
                return running

            return lax.fori_loop(0, 8, add, jnp.zeros((16, 128), F32))

        mean = total(lambda h: source[half, h].astype(F32)) * (1.0 / 128)

        def square(h):
            center = source[half, h].astype(F32) - mean
            return center * center

        inverse = lax.rsqrt(total(square) * (1.0 / 128) + EPS)

        @pl.loop(0, 8)
        def _(hz):
            for k in range(16):
                h = hz * 16 + k
                mixed = (source[half, h].astype(F32) - mean) * inverse * og_ref[update, h]
                stage[pl.ds(pl.multiple_of(h * PITCH + half * 16, 8), 16), :] = mixed

        weight = wt[update, 5]

        for step in range(per_half):
            mixed = jnp.concatenate(
                [
                    stage[pl.ds(half * 16 + step * tiles + t, 128, stride=PITCH), :]
                    for t in range(tiles)
                ],
                axis=1,
            ).astype(BF)
            change = jnp.dot(weight, mixed, preferred_element_type=F32)
            here = pl.ds(half * 2048 + step * LANES, LANES)
            total_here = old[:, here].astype(F32) + gate[:, here] * change
            if update == 0:
                state[:, here] = total_here.astype(BF)
                continue
            for t in range(tiles):
                row_of_j = half * 16 + step * tiles + t
                stage[pl.ds(row_of_j, 128, stride=PITCH), :] = total_here[:, t * 128 : (t + 1) * 128].T
        if update == 1:
            rows = pl.ds(half * 16, 16)

            @pl.loop(0, 16)
            def _(step):
                for k in range(8):
                    i = step * 8 + k
                    begin = pl.multiple_of(i * PITCH + half * 16, 8)
                    out_ref[i, rows, :] = stage[pl.ds(begin, 16), :].astype(BF)

    def scope(name, run, *args):
        with jax.named_scope(name):
            run(*args)

    b = buffers[0]
    for k in range(3):
        loads[k].wait()
    for p in range(4):
        turn_weight(0, p, pw_ref[0, p])
    for half in range(2):
        scope("load", load, half)
        scope("normalise", normalise, 0, start, half)
        scope("project", project, 0, 1, b["first"], half)
        if half == 0:
            with jax.named_scope("barrier"):
                pl.semaphore_wait(barrier, 255)
        scope("send_first", send_right, f"first{half}", b["first"], half)
    for half in range(2):
        scope("project", project, 0, 0, b["last"], half)
        scope("send_last", send_left, f"last{half}", b["last"], half)
    for k in range(3, 6):
        loads[k].wait()
    for u in range(2):
        if u == 1:
            for p in range(4):
                turn_weight(1, p, pw_ref[1, p])
        turn_weight(u, 4, gw_ref[u])
        turn_weight(u, 5, ow_ref[u])
    for half in range(2):
        scope("gates", gates, 0, half)

    def swap(update):
        whole = buffers[update]["all_first"]
        own = whole.at[:, :, :, core] if update == 0 else whole.at[:, :, :, :, :, core]
        copy(update, "swap", own, own, device(x, y, z, other)).start()
        arrived(update, "swap")

    for half in range(2):
        arrived(0, f"first{half}")
    swap(0)
    scope("turn_right", turn_right)
    for half in range(2):
        arrived(0, f"last{half}")
        scope("contract", contract_outgoing, half)
        for yq in range(2):
            scope("send_tri", send_rows, half, yq)

    b = buffers[1]
    for half in range(2):
        arrived(0, f"tri{half}")
        scope("finish", finish, 0, half, start)
        scope("normalise", normalise, 1, state, half)
        scope("project", project, 1, 0, b["first"], half)
        scope("send_first", send_near, "first", half)
    scope("unfold", unfold)
    for half in range(2):
        scope("normalise", normalise, 1, start, half)
        scope("project", project, 1, 1, b["last"], half)
    for half in range(2):
        scope("gates", gates, 1, half)
    for half in range(2):
        arrived(1, f"first{half}")
        scope("pass", pass_left, half)
    for half in range(2):
        scope("send_last", send_near, "last", half)
    for half in range(2):
        arrived(1, f"pass{half}")
    swap(1)
    scope("turn_left", turn_left)
    for half in range(2):
        arrived(1, f"last{half}")
        for step in range(4):
            scope("send_tri", send_triangle, half, step)
    for half in range(2):
        arrived(1, f"tri{half}")
        scope("finish", finish, 1, half, start)

    for u in range(2):
        for name in FLOWS:
            if u == 1 or not name.startswith("pass"):
                waits(u, name, "send")


def local(pair_rep, proj_weight, gate_weight, out_weight, in_gain, out_gain):
    inputs = [
        pltpu.with_memory_space_constraint(array, pltpu.HBM)
        for array in (pair_rep, proj_weight, gate_weight, out_weight, in_gain, out_gain)
    ]
    buffers = [pltpu.VMEM(shape, BF) for u in range(2) for shape in scratch_of(u).values()]
    return pl.pallas_call(
        kernel,
        out_shape=jax.ShapeDtypeStruct((128, 32, 128), BF),
        in_specs=[pl.BlockSpec(memory_space=pltpu.HBM)] * 6,
        out_specs=pl.BlockSpec(memory_space=pltpu.VMEM),
        scratch_shapes=buffers
        + [
            pltpu.VMEM((2, 6, 128, 128), BF),
            pltpu.VMEM((128, 4096), BF),
            pltpu.VMEM((128, 4096), F32),
            pltpu.VMEM((128, 4096), BF),
            pltpu.VMEM((128, 4096), BF),
            pltpu.VMEM((128 * PITCH, 128), F32),
            pltpu.VMEM((2, 32, 16, 1024), BF),
            pltpu.VMEM((2, 8, 32, 2, 16, 128), BF),
            pltpu.VMEM((512, 16, 128), BF),
            pltpu.SemaphoreType.DMA((2 * len(FLOWS),)),
            pltpu.SemaphoreType.DMA((2 * len(FLOWS),)),
            pltpu.VMEM((128, 32, 128), BF),
            pltpu.VMEM((2, 4, 128, 128), BF),
            pltpu.VMEM((2, 128, 128), BF),
            pltpu.VMEM((2, 128, 128), BF),
            pltpu.VMEM((2, 128), F32),
            pltpu.SMEM((2, 128), F32),
            pltpu.SemaphoreType.DMA((6,)),
        ],
        compiler_params=pltpu.CompilerParams(
            collective_id=0, has_side_effects=True, vmem_limit_bytes=44 * 1024 * 1024
        ),
    )(*inputs)


def solution(mesh):
    placed = (P("row", "col", None), P(), P(), P(), P(), P())
    return jax.shard_map(
        local, mesh=mesh, in_specs=placed, out_specs=P("row", "col", None), check_vma=False
    )
```
